256 devices in a mesh: dp: 32 (over z, y), mp: 8 (over x, core).
Axes of the slice: x: 4, y: 4, z: 8, core: 2. Of those that a mesh axis runs over, the one named last changes fastest.
Arguments:
- residual_input: bfloat16 [8192, 5120], P('dp', 'mp'), may hold values from -6 to 6
- cotangent: bfloat16 [8192, 5120], P('dp', 'mp'), may hold values from -0.6 to 0.6
- lengths: int32 [32], P('dp'), may hold values from 64 to 256
- norm_gain_vector: bfloat16 [5120], replicated, may hold values from 0.5 to 1.5
- gate_projection_weight: bfloat16 [5120, 6912], P('dp', 'mp'), may hold values from -0.078125 to 0.078125
- up_projection_weight: bfloat16 [5120, 6912], P('dp', 'mp'), may hold values from -0.078125 to 0.078125
- down_projection_weight: bfloat16 [5120, 6912], P('dp', 'mp'), may hold values from -0.078125 to 0.078125
- up_adapter_first: bfloat16 [5120, 16], replicated, may hold values from -0.078125 to 0.078125
- up_adapter_second: bfloat16 [16, 6912], P(None, 'mp'), may hold values from -0.29882812 to 0.29882812
- down_adapter_first: bfloat16 [6912, 16], P('mp'), may hold values from -0.078125 to 0.078125
- down_adapter_second: bfloat16 [16, 5120], replicated, may hold values from -0.29882812 to 0.29882812
Outputs:
- up_first_gradient: float32 [5120, 16], P('dp')
- up_second_gradient: float32 [16, 6912], P(None, ('mp', 'dp'))
- down_first_gradient: float32 [6912, 16], P(('mp', 'dp'))
- down_second_gradient: float32 [16, 5120], P(None, 'dp')
The draws below stay inside these ranges and needn't reach their ends.
All inputs are finite; a program needn't handle non-finite values.
Results may differ from the reference program's by a relative error of at most 0.0061.
Values may be sent and summed in bfloat16 or wider, within the bound.
A program may use at most 128 MiB of HBM per device.

```python
import math
import jax
import jax.numpy as jnp
from jax import lax

MODEL_WIDTH = 5120
HIDDEN_SHARD = 6912
ADAPTER_RANK = 16
SEQ = 256
BATCH = 32
TOKENS = 8192


def draw_cotangent(key, part):
    row_key = jax.random.fold_in(key, 11)
    value_key = jax.random.fold_in(key, 23)
    spread = jnp.exp(jax.random.uniform(row_key, (BATCH, 1, 1), jnp.float32, 0.0, math.log(10.0)))
    values = jnp.clip(jax.random.normal(value_key, (BATCH, SEQ, MODEL_WIDTH), jnp.float32), -6.0, 6.0)
    return (0.01 * spread * values).reshape(BATCH * SEQ, MODEL_WIDTH).astype(jnp.bfloat16)


def touch_ends(result, key, smallest, top_value):
    shape = result.shape
    place = [jax.random.randint(jax.random.fold_in(key, axis), (), 0, shape[axis]) for axis in range(len(shape))]
    result = result.at[tuple(place)].set(smallest)
    longest = shape.index(max(shape))
    place[longest] = (place[longest] + 1) % shape[longest]
    return result.at[tuple(place)].set(top_value)


def level_of(own_key, dims, split, smallest, high):
    level = 1.0
    for axis_at, parts in split:
        steps = jax.random.uniform(jax.random.fold_in(jax.random.fold_in(own_key, 6), axis_at), (parts,), jnp.float32, smallest / len(split), high / len(split))
        level = level * jnp.repeat(jnp.exp(steps), dims[axis_at] // parts).reshape((-1,) + (1,) * (len(dims) - 1 - axis_at))
    return level


def gaussian(rng, dims, scale, bound, pieces=(), kind=jnp.bfloat16):
    factor_of = level_of(rng, dims, pieces, -0.22, 0.18) if pieces else 1.0
    entries = jax.random.normal(rng, dims, jnp.float32) * scale * factor_of
    return jnp.minimum(jnp.maximum(entries, -bound), bound).astype(kind)


def setup_inputs(seed: int = 0) -> dict:
    seeds = jax.random.split(jax.random.key(seed), 12)
    residual_input = gaussian(seeds[0], (TOKENS, MODEL_WIDTH), 1.0, 6.0, ((0, 32), (1, 8)))
    cotangent = draw_cotangent(jax.random.fold_in(seeds[11], 71), 0)
    lengths = touch_ends(jax.random.randint(seeds[2], (BATCH,), SEQ // 4, SEQ + 1), jax.random.fold_in(seeds[2], 1), SEQ // 4, SEQ).astype(jnp.int32)
    norm_gain_vector = jnp.clip(1.0 + 0.1 * jax.random.normal(seeds[3], (MODEL_WIDTH,), jnp.float32), 0.5, 1.5).astype(jnp.bfloat16)
    gate_projection_weight = gaussian(seeds[4], (MODEL_WIDTH, HIDDEN_SHARD), MODEL_WIDTH ** -0.5, 0.078125, ((0, 32), (1, 8)))
    up_projection_weight = gaussian(seeds[5], (MODEL_WIDTH, HIDDEN_SHARD), MODEL_WIDTH ** -0.5, 0.078125, ((0, 32), (1, 8)))
    down_projection_weight = gaussian(seeds[6], (MODEL_WIDTH, HIDDEN_SHARD), HIDDEN_SHARD ** -0.5, 0.078125, ((0, 32), (1, 8)))
    up_adapter_first = gaussian(seeds[7], (MODEL_WIDTH, ADAPTER_RANK), MODEL_WIDTH ** -0.5, 0.078125)
    up_adapter_second = gaussian(seeds[8], (ADAPTER_RANK, HIDDEN_SHARD), 0.05, 0.29882812, ((1, 8),))
    down_adapter_first = gaussian(seeds[9], (HIDDEN_SHARD, ADAPTER_RANK), HIDDEN_SHARD ** -0.5, 0.078125, ((0, 8),))
    down_adapter_second = gaussian(seeds[10], (ADAPTER_RANK, MODEL_WIDTH), 0.05, 0.29882812)
    return {"residual_input": residual_input, "cotangent": cotangent, "lengths": lengths, "norm_gain_vector": norm_gain_vector, "gate_projection_weight": gate_projection_weight, "up_projection_weight": up_projection_weight, "down_projection_weight": down_projection_weight, "up_adapter_first": up_adapter_first, "up_adapter_second": up_adapter_second, "down_adapter_first": down_adapter_first, "down_adapter_second": down_adapter_second}


norm_eps = 1e-06
adapter_scale = 2.0
clip_coefficient = 0.005

def reference(residual_input, cotangent, lengths, norm_gain_vector, gate_projection_weight, up_projection_weight, down_projection_weight, up_adapter_first, up_adapter_second, down_adapter_first, down_adapter_second):
    single_float = jnp.float32
    half_precision = jnp.bfloat16
    clip_limit = clip_coefficient * math.sqrt(2.0 * ADAPTER_RANK * (MODEL_WIDTH + HIDDEN_SHARD))
    positions = jnp.arange(SEQ, dtype=jnp.int32)
    live = (positions[None, :] < lengths[:, None]).astype(single_float).reshape(TOKENS, 1)
    output_gradient = (cotangent.astype(single_float) * live).astype(half_precision)
    wide = residual_input.astype(single_float)
    inverse = lax.rsqrt(lax.optimization_barrier(jnp.mean(wide * wide, axis=1, keepdims=True)) + norm_eps)
    normalized_input = (wide * inverse * norm_gain_vector.astype(single_float)).astype(half_precision)
    up_adapter_latent = jnp.dot(normalized_input, up_adapter_first, preferred_element_type=single_float).astype(half_precision)
    gate = jnp.dot(normalized_input, gate_projection_weight, preferred_element_type=single_float)
    up_activation = jnp.dot(normalized_input, up_projection_weight, preferred_element_type=single_float) + adapter_scale * jnp.dot(up_adapter_latent, up_adapter_second, preferred_element_type=single_float)
    gate_act = jax.nn.silu(gate)
    hidden_activation = (gate_act * up_activation).astype(half_precision)
    down_adapter_latent = jnp.dot(hidden_activation, down_adapter_first, preferred_element_type=single_float).astype(half_precision)
    backward_adapter = jnp.dot(output_gradient, down_adapter_second.T, preferred_element_type=single_float).astype(half_precision)
    hidden_gradient = jnp.dot(output_gradient, down_projection_weight, preferred_element_type=single_float) + adapter_scale * jnp.dot(backward_adapter, down_adapter_first.T, preferred_element_type=single_float)
    up_gradient = (hidden_gradient * gate_act).astype(half_precision)
    up_adapter_hidden = jnp.dot(up_gradient, up_adapter_second.T, preferred_element_type=single_float).astype(half_precision)

    def split_parts(values):
        return values.astype(single_float).reshape(BATCH, SEQ, values.shape[1])
    example_down_second = adapter_scale * jnp.einsum('kox,kou->kxu', split_parts(down_adapter_latent), split_parts(output_gradient))
    example_down_first = adapter_scale * jnp.einsum('yze,yzx->yex', split_parts(hidden_activation), split_parts(backward_adapter))
    example_up_second = adapter_scale * jnp.einsum('uml,umk->ulk', split_parts(up_adapter_latent), split_parts(up_gradient))
    example_up_first = adapter_scale * jnp.einsum('mju,mjl->mul', split_parts(normalized_input), split_parts(up_adapter_hidden))
    squares = lax.optimization_barrier(jnp.sum(example_down_second * example_down_second, axis=(1, 2))) + lax.optimization_barrier(jnp.sum(example_down_first * example_down_first, axis=(1, 2)))
    squares = squares + lax.optimization_barrier(jnp.sum(example_up_second * example_up_second, axis=(1, 2))) + lax.optimization_barrier(jnp.sum(example_up_first * example_up_first, axis=(1, 2)))
    factor = jnp.minimum(1.0, clip_limit / (jnp.sqrt(squares) + 1e-06))
    up_first_gradient = jnp.einsum('b,bdr->dr', factor, example_up_first)
    up_second_gradient = jnp.einsum('b,brf->rf', factor, example_up_second)
    down_first_gradient = jnp.einsum('b,bfr->fr', factor, example_down_first)
    down_second_gradient = jnp.einsum('b,brd->rd', factor, example_down_second)
    return (up_first_gradient, up_second_gradient, down_first_gradient, down_second_gradient)
```

```python
import math

import jax
import jax.numpy as jnp
from jax import lax
from jax.experimental import pallas as pl
from jax.experimental.pallas import tpu as pltpu
from jax.sharding import PartitionSpec as P

MODEL_WIDTH = 5120
HIDDEN_SHARD = 6912
ADAPTER_RANK = 16

norm_eps = 1e-06
adapter_scale = 2.0
clip_coefficient = 0.005

NZ, NY, NX, NC = 8, 4, 4, 2
NMP = NX * NC
NDP = NZ * NY
ROWS = 160
KLEN = ROWS * NZ
SEQ = 256
COLS = 864
WIDE = 896
HALF = ROWS // 2

PIECES = ((0, 0, 0, 896), (1, 0, 0, 896), (2, 1, 0, 512), (2, 1, 512, 384))
RING = (((0, 0), (0, 1), (1, 0), (1, 1), (2, 0), (2, 1), (3, 0)), ((0, 0), (0, 1), (1, 0), (1, 1), (2, 0), (2, 1), (3, 1)))
MESH = pl.DeviceIdType.MESH
BF, F32 = jnp.bfloat16, jnp.float32


def contract_row_dims(left, right):
    return lax.dot_general(left, right, (((0,), (0,)), ((), ())), preferred_element_type=F32)


def contract_columns(left, right):
    return lax.dot_general(left, right, (((1,), (1,)), ((), ())), preferred_element_type=F32)


def remote(src, dst, send, recv, dp, mp):
    return pltpu.make_async_remote_copy(
        src_ref=src, dst_ref=dst, send_sem=send, recv_sem=recv, device_id={"dp": dp, "mp": mp}, device_id_type=MESH
    )


def signal(sem, dp, mp):
    pl.semaphore_signal(sem, inc=1, device_id={"dp": dp, "mp": mp}, device_id_type=MESH)


def products_kernel(
    at, wb, ps, c_out, p_out, a_all, b_all, cs2, cs1, cr2, cr1, p_all,
    bs, br, ays, ayr, loc, axs, axr, ads, adr, c2s, c2r, c1s, c1r, pss, psr,
):
    d, m = lax.axis_index("dp"), lax.axis_index("mp")
    z, y, x, c = d // NY, lax.rem(d, NY), m // NC, lax.rem(m, NC)

    def dp_of(zz, yy):
        return lax.rem(zz, NZ) * NY + lax.rem(yy, NY)

    def mp_of(xx, cc):
        return lax.rem(xx, NX) * NC + cc

    up_z, down_z = dp_of(z + 1, y), dp_of(z + NZ - 1, y)
    up_y, down_y = dp_of(z, y + 1), dp_of(z, y + NY - 1)
    up_x, down_x = mp_of(x + 1, c), mp_of(x + NX - 1, c)
    far_x = mp_of(x + 2, c)
    twin = mp_of(x, 1 - c)

    bar = pltpu.get_barrier_semaphore()
    signal(bar, up_z, m)
    signal(bar, down_z, m)
    for k in range(1, NY):
        signal(bar, dp_of(z, y + k), m)
    for k in range(1, NMP):
        signal(bar, d, lax.rem(m + k, NMP))
    pl.semaphore_wait(bar, 2 + NY - 1 + NMP - 1)

    def rows_of(zz, h, n):
        return pl.ds(pl.multiple_of(zz * ROWS + h * HALF, 16), n)

    def ring_copy(p, way, i):
        w, _, c0, n = PIECES[p]
        s, h = RING[way][i]
        src_z = lax.rem(z + (NZ - s if way == 0 else s), NZ)
        cols = pl.ds(c0, n)
        here = wb.at[w, pl.ds(h * HALF, HALF), cols] if s == 0 else b_all.at[w, rows_of(src_z, h, HALF), cols]
        there = b_all.at[w, rows_of(src_z, h, HALF), cols]
        return remote(here, there, bs.at[p, way, i], br.at[p, way, i], up_z if way == 0 else down_z, m)

    def ring_issue(p, i):
        for way in range(2):
            s, h = RING[way][i]
            if s:
                ring_copy(p, way, 2 * (s - 1) + h).wait_recv()
            ring_copy(p, way, i).start()

    def ring_finish(p):
        for way in range(2):
            for i in (5, 6) if way == 0 else (4, 6):
                ring_copy(p, way, i).wait_recv()

    def feats(mm):
        return pl.ds(pl.multiple_of(mm * ROWS, 16), ROWS)

    def y_copy(a, k):
        yy = lax.rem(y + k, NY)
        return remote(at.at[yy, a], a_all.at[y, a, feats(m), :], ays.at[a, k - 1], ayr.at[a, k - 1], dp_of(z, yy), m)

    def own_copy(a):
        return pltpu.make_async_copy(at.at[y, a], a_all.at[y, a, feats(m), :], loc.at[a])

    def block(a, mm, e0, ne):
        return a_all.at[pl.ds(e0, ne), a, feats(mm), :]

    def x_copy(a, i):
        mm, e0, ne, to = ((m, 0, 4, up_x), (m, 0, 4, down_x), (down_x, 0, 2, up_x), (up_x, 2, 2, down_x))[i]
        return remote(block(a, mm, e0, ne), block(a, mm, e0, ne), axs.at[a, i], axr.at[a, i], d, to)

    def core_copy(a, i):
        mm, e0, ne = ((m, 0, 4), (down_x, 0, 4), (up_x, 0, 4), (far_x, 0, 2), (far_x, 2, 2))[i]
        return remote(block(a, mm, e0, ne), block(a, mm, e0, ne), ads.at[a, i], adr.at[a, i], d, twin)

    def tokens_start(a):
        for k in (2, 1, 3):
            y_copy(a, k).start()
        own_copy(a).start()

    def tokens_x(a):
        own_copy(a).wait()
        for k in (1, 2, 3):
            y_copy(a, k).wait_recv()
        x_copy(a, 0).start()
        x_copy(a, 1).start()
        core_copy(a, 0).start()

    def tokens_on(a):
        x_copy(a, 0).wait_recv()
        x_copy(a, 2).start()
        x_copy(a, 1).wait_recv()
        x_copy(a, 3).start()
        core_copy(a, 1).start()
        core_copy(a, 2).start()

    def tokens_last(a):
        x_copy(a, 2).wait_recv()
        core_copy(a, 3).start()
        x_copy(a, 3).wait_recv()
        core_copy(a, 4).start()

    def tokens_done(a):
        for i in range(5):
            core_copy(a, i).wait_recv()

    def product(p, t, store):
        w, a, c0, n = PIECES[p]

        def tile(lo, size):
            acc = lax.dot_general(
                a_all[t, a], b_all[w, :, pl.ds(lo, size)], (((0,), (0,)), ((), ())), preferred_element_type=F32
            )
            store(w, lo, size, acc)

        def step(i, carry):
            tile(pl.multiple_of(c0 + i * 256, 128), 256)
            return carry

        lax.fori_loop(0, n // 256, step, 0)
        if n % 256:
            tile(c0 + n - n % 256, n % 256)

    def half_copy(p, way):
        w, _, c0, n = PIECES[p]
        cols = pl.ds(c0, n)
        return remote(
            cs2.at[w, way, :, cols], cr2.at[w, way, :, cols], c2s.at[p, way], c2r.at[p, way], up_y if way == 0 else down_y, m
        )

    def full_copy(p, way, h):
        w, _, c0, n = PIECES[p]
        part = (way, pl.ds(h * 128, 128), pl.ds(c0, n))
        return remote(
            cs1.at[(w, *part)], cr1.at[(w, *part)], c1s.at[p, way, h], c1r.at[p, way, h], up_y if way == 0 else down_y, m
        )

    def unit_far(p):
        def store(w, lo, size, acc):
            v = acc.astype(BF)
            cs2[w, 0, :, pl.ds(lo, size)] = v[:128]
            cs2[w, 1, :, pl.ds(lo, size)] = v[128:]

        product(p, lax.rem(y + 2, NY), store)
        half_copy(p, 0).start()
        half_copy(p, 1).start()

    def unit_near(p, way):
        def store(w, lo, size, acc):
            cs1[w, way, :, pl.ds(lo, size)] = acc.astype(BF)

        product(p, lax.rem(y + (1 if way == 0 else NY - 1), NY), store)
        full_copy(p, way, 1 - way).start()

    def unit_pass(p):
        w, _, c0, n = PIECES[p]
        for way in range(2):
            half_copy(p, way).wait_recv()
            at_rows, cols = pl.ds(way * 128, 128), pl.ds(c0, n)
            total = cs1[w, way, at_rows, cols].astype(F32) + cr2[w, way, :, cols].astype(F32)
            cs1[w, way, at_rows, cols] = total.astype(BF)
            full_copy(p, way, way).start()

    def unit_own(p):
        def store(w, lo, size, acc):
            c_out[w, :, pl.ds(lo, size)] = acc

        product(p, y, store)

    def unit_sum(p):
        w, _, c0, n = PIECES[p]
        cols = pl.ds(c0, n)
        for way in range(2):
            for h in range(2):
                full_copy(p, way, h).wait_recv()
        c_out[w, :, cols] += cr1[w, 0, :, cols].astype(F32) + cr1[w, 1, :, cols].astype(F32)

    def p_copy(k):
        return remote(ps, p_all.at[m], pss.at[k - 1], psr.at[k - 1], d, lax.rem(m + k, NMP))

    def own_rows():
        for w in range(3):
            b_all[w, rows_of(z, 0, ROWS), :] = wb[w]

    def units(p):
        return [
            lambda: unit_far(p),
            lambda: unit_near(p, 0),
            lambda: unit_near(p, 1),
            lambda: unit_pass(p),
            lambda: unit_own(p),
        ]

    plan = {(p, i): [] for p in range(4) for i in range(7)}
    plan[0, 0] += [lambda: tokens_start(0), lambda: tokens_start(1)]
    plan[0, 1] += [lambda: [p_copy(k).start() for k in range(1, NMP)], own_rows]
    plan[0, 3] += [lambda: tokens_x(0)]
    plan[0, 6] += [lambda: tokens_on(0), lambda: tokens_x(1)]
    plan[1, 1] += [lambda: tokens_last(0)]
    plan[1, 2] += [lambda: ring_finish(0), lambda: tokens_done(0)]
    for j, u in enumerate(units(0)):
        plan[1, 2 + j] += [u]
    plan[1, 4] += [lambda: tokens_on(1)]
    plan[1, 6] += [lambda: tokens_last(1)]
    plan[2, 2] += [lambda: unit_sum(0), lambda: ring_finish(1)]
    for j, u in enumerate(units(1)):
        plan[2, 2 + j] += [u]
    plan[3, 2] += [lambda: unit_sum(1), lambda: ring_finish(2), lambda: tokens_done(1)]
    for j, u in enumerate(units(2)):
        plan[3, 2 + j] += [u]

    for p in range(4):
        for i in range(7):
            ring_issue(p, i)
            for u in plan[p, i]:
                u()
    ring_finish(3)
    for u in units(3):
        u()
    unit_sum(2)
    unit_sum(3)
    p_all[m] = ps[...]
    for k in range(1, NMP):
        p_copy(k).wait_recv()
    p_out[...] = jnp.sum(p_all[...], axis=0)

    for p in range(4):
        for way in range(2):
            for i in range(7):
                ring_copy(p, way, i).wait_send()
            half_copy(p, way).wait_send()
            for h in range(2):
                full_copy(p, way, h).wait_send()
    for a in range(2):
        for k in (1, 2, 3):
            y_copy(a, k).wait_send()
        for i in range(4):
            x_copy(a, i).wait_send()
        for i in range(5):
            core_copy(a, i).wait_send()
    for k in range(1, NMP):
        p_copy(k).wait_send()


def products(at, wb, ps):
    vmem = pl.BlockSpec(memory_space=pltpu.VMEM)
    dma = pltpu.SemaphoreType.DMA
    return pl.pallas_call(
        products_kernel,
        out_shape=(jax.ShapeDtypeStruct((3, SEQ, WIDE), F32), jax.ShapeDtypeStruct((8, SEQ), F32)),
        in_specs=[vmem] * 3,
        out_specs=(vmem, vmem),
        scratch_shapes=[
            pltpu.VMEM((NY, 2, KLEN, SEQ), BF),
            pltpu.VMEM((3, KLEN, WIDE), BF),
            pltpu.VMEM((3, 2, 128, WIDE), BF),
            pltpu.VMEM((3, 2, SEQ, WIDE), BF),
            pltpu.VMEM((3, 2, 128, WIDE), BF),
            pltpu.VMEM((3, 2, SEQ, WIDE), BF),
            pltpu.VMEM((NMP, 8, SEQ), F32),
            dma((4, 2, 7)),
            dma((4, 2, 7)),
            dma((2, 3)),
            dma((2, 3)),
            dma((2,)),
            dma((2, 4)),
            dma((2, 4)),
            dma((2, 5)),
            dma((2, 5)),
            dma((4, 2)),
            dma((4, 2)),
            dma((4, 2, 2)),
            dma((4, 2, 2)),
            dma((NMP - 1,)),
            dma((NMP - 1,)),
        ],
        compiler_params=pltpu.CompilerParams(collective_id=0, has_side_effects=True),
        name="products",
    )(at, wb, ps)


def group_sum_kernel(v, out, land, ss, rs):
    d, m = lax.axis_index("dp"), lax.axis_index("mp")
    bar = pltpu.get_barrier_semaphore()
    for k in range(1, NMP):
        signal(bar, d, lax.rem(m + k, NMP))
    pl.semaphore_wait(bar, NMP - 1)

    def copy(k):
        return remote(v, land.at[m], ss.at[k - 1], rs.at[k - 1], d, lax.rem(m + k, NMP))

    for k in range(1, NMP):
        copy(k).start()
    land[m] = v[...]
    for k in range(1, NMP):
        copy(k).wait_recv()
    out[...] = jnp.sum(land[...], axis=0)
    for k in range(1, NMP):
        copy(k).wait_send()


def group_sum(v, cid):
    vmem = pl.BlockSpec(memory_space=pltpu.VMEM)
    dma = pltpu.SemaphoreType.DMA
    return pl.pallas_call(
        group_sum_kernel,
        out_shape=jax.ShapeDtypeStruct(v.shape, F32),
        in_specs=[vmem],
        out_specs=vmem,
        scratch_shapes=[pltpu.VMEM((NMP, *v.shape), F32), dma((NMP - 1,)), dma((NMP - 1,))],
        compiler_params=pltpu.CompilerParams(collective_id=cid, has_side_effects=True),
        name=f"group_sum_{cid}",
    )(v)


def final_kernel(u, s, u_out, s_out, u_land, s_land, us, ur, ss, sr):
    d, m = lax.axis_index("dp"), lax.axis_index("mp")
    z, y = d // NY, lax.rem(d, NY)
    bar = pltpu.get_barrier_semaphore()

    def greet(k, carry):
        signal(bar, lax.rem(d + k, NDP), m)
        return carry

    lax.fori_loop(1, NDP, greet, 0)

    def is_self(dd, mm):
        return jnp.logical_and(dd == d, mm == m)

    def greet_source(k, carry):
        @pl.when(jnp.logical_not(is_self(k, z)))
        def _():
            signal(bar, k, z)

        return carry

    lax.fori_loop(0, NDP, greet_source, 0)
    mine = (z == m).astype(jnp.int32)
    pl.semaphore_wait(bar, NDP - 1 + NDP - mine)

    def u_copy(k):
        yy, mm = k // NMP, lax.rem(k, NMP)
        dd = m * NY + yy
        return remote(u.at[yy], u_land.at[d], us.at[k], ur.at[d], dd, mm), is_self(dd, mm)

    def s_copy(k):
        dd = lax.rem(d + k, NDP)
        return remote(s.at[dd], s_land.at[d], ss.at[k], sr.at[d], dd, m)

    def u_start(k, carry):
        copy, own = u_copy(k)

        @pl.when(jnp.logical_not(own))
        def _():
            copy.start()

        return carry

    def s_start(k, carry):
        s_copy(k).start()
        return carry

    lax.fori_loop(0, NDP, u_start, 0)
    lax.fori_loop(1, NDP, s_start, 0)
    s_land[d] = s[d]

    @pl.when(z == m)
    def _():
        u_land[d] = u[y]

    def u_wait(k, carry):
        @pl.when(jnp.logical_not(is_self(k, z)))
        def _():
            remote(u.at[0], u_land.at[k], us.at[0], ur.at[k], d, m).wait_recv()

        return carry

    def s_wait(k, carry):
        dd = lax.rem(d + k, NDP)
        remote(s.at[0], s_land.at[dd], ss.at[0], sr.at[dd], d, m).wait_recv()
        return carry

    lax.fori_loop(0, NDP, u_wait, 0)
    lax.fori_loop(1, NDP, s_wait, 0)
    u_out[...] = jnp.sum(u_land[...].astype(F32), axis=0)
    s_out[...] = jnp.sum(s_land[...], axis=0)

    def sent(k, carry):
        copy, own = u_copy(k)

        @pl.when(jnp.logical_not(own))
        def _():
            copy.wait_send()

        return carry

    def s_sent(k, carry):
        s_copy(k).wait_send()
        return carry

    lax.fori_loop(0, NDP, sent, 0)
    lax.fori_loop(1, NDP, s_sent, 0)


def final_sums(u, s):
    vmem = pl.BlockSpec(memory_space=pltpu.VMEM)
    dma = pltpu.SemaphoreType.DMA
    return pl.pallas_call(
        final_kernel,
        out_shape=(jax.ShapeDtypeStruct(u.shape[1:], F32), jax.ShapeDtypeStruct(s.shape[1:], F32)),
        in_specs=[vmem, vmem],
        out_specs=(vmem, vmem),
        scratch_shapes=[
            pltpu.VMEM((NDP, *u.shape[1:]), u.dtype),
            pltpu.VMEM(s.shape, s.dtype),
            dma((NDP,)),
            dma((NDP,)),
            dma((NDP,)),
            dma((NDP,)),
        ],
        compiler_params=pltpu.CompilerParams(collective_id=3, has_side_effects=True),
        name="final_sums",
    )(u, s)


def per_device(
    residual_input,
    cotangent,
    lengths,
    norm_gain_vector,
    gate_projection_weight,
    up_projection_weight,
    down_projection_weight,
    up_adapter_first,
    up_adapter_second,
    down_adapter_first,
    down_adapter_second,
):
    clip_limit = clip_coefficient * math.sqrt(2.0 * ADAPTER_RANK * (MODEL_WIDTH + HIDDEN_SHARD))
    d, m = lax.axis_index("dp"), lax.axis_index("mp")
    features = residual_input.shape[1]
    gain = lax.dynamic_slice(norm_gain_vector, (m * features,), (features,)).astype(F32)[None, :]
    positions = lax.broadcasted_iota(jnp.int32, (SEQ, 1), 0)
    live = (positions < lengths[0]).astype(F32)
    output_gradient = (cotangent.astype(F32) * live).astype(BF)
    wide = residual_input.astype(F32)
    scaled = (wide * gain).astype(BF)
    at = jnp.stack([scaled.T.reshape(NY, ROWS, SEQ), output_gradient.T.reshape(NY, ROWS, SEQ)], axis=1)
    ps = jnp.broadcast_to(jnp.sum(wide * wide, axis=1)[None, :], (8, SEQ))
    first = lax.dynamic_slice(up_adapter_first, (d * ROWS, 0), (ROWS, ADAPTER_RANK))
    second = lax.dynamic_slice(down_adapter_second, (0, d * ROWS), (ADAPTER_RANK, ROWS)).T
    rest = jnp.zeros((ROWS, WIDE - COLS - ADAPTER_RANK), BF)
    wb = jnp.stack(
        [
            jnp.concatenate([gate_projection_weight, jnp.zeros_like(first), rest], axis=1),
            jnp.concatenate([up_projection_weight, first, rest], axis=1),
            jnp.concatenate([down_projection_weight, second, rest], axis=1),
        ]
    )
    c_all, squares_of_rows = products(at, wb, ps)
    inverse = lax.rsqrt(squares_of_rows[0] * (1.0 / MODEL_WIDTH) + norm_eps)[:, None]
    gate = c_all[0, :, :COLS] * inverse
    up_frozen_output = c_all[1, :, :COLS] * inverse
    up_adapter_latent = (c_all[1, :, COLS : COLS + ADAPTER_RANK] * inverse).astype(BF)
    backward_frozen = c_all[2, :, :COLS]
    backward_adapter = c_all[2, :, COLS : COLS + ADAPTER_RANK].astype(BF)

    up_activation = up_frozen_output + adapter_scale * jnp.dot(
        up_adapter_latent, up_adapter_second, preferred_element_type=F32
    )
    gate_act = jax.nn.silu(gate)
    hidden_activation = (gate_act * up_activation).astype(BF)
    hidden_gradient = backward_frozen + adapter_scale * contract_columns(backward_adapter, down_adapter_first)
    up_gradient = (hidden_gradient * gate_act).astype(BF)
    down_partial = lax.dot_general(
        down_adapter_first, hidden_activation, (((0,), (1,)), ((), ())), preferred_element_type=F32
    )
    up_partial = contract_columns(up_adapter_second, up_gradient)
    down_first_gradient = adapter_scale * contract_row_dims(hidden_activation, backward_adapter)
    up_second_gradient = adapter_scale * contract_row_dims(up_gradient, up_adapter_latent)
    shared = jnp.sum(down_first_gradient * down_first_gradient) + jnp.sum(up_second_gradient * up_second_gradient)
    latents = group_sum(
        jnp.concatenate([down_partial, up_partial, jnp.broadcast_to(shared, (8, SEQ))], axis=0), 1
    )
    down_adapter_latent = latents[:ADAPTER_RANK].astype(BF)
    up_adapter_hidden = latents[ADAPTER_RANK : 2 * ADAPTER_RANK].astype(BF)
    normalized = (wide * inverse * gain).astype(BF)
    up_first_gradient = adapter_scale * lax.dot_general(
        normalized, up_adapter_hidden, (((0,), (1,)), ((), ())), preferred_element_type=F32
    )
    down_second_gradient = adapter_scale * lax.dot_general(
        output_gradient, down_adapter_latent, (((0,), (1,)), ((), ())), preferred_element_type=F32
    )
    owned = jnp.sum(up_first_gradient * up_first_gradient) + jnp.sum(down_second_gradient * down_second_gradient)
    owned_total = group_sum(jnp.broadcast_to(owned, (8, 128)), 2)[0, 0]
    factor = jnp.minimum(1.0, clip_limit / (jnp.sqrt(owned_total + latents[2 * ADAPTER_RANK, 0]) + 1e-06))
    u = (factor * jnp.concatenate([up_first_gradient, down_second_gradient], axis=1)).astype(BF)
    u = u.reshape(NY, ROWS * 2 * ADAPTER_RANK // 128, 128)
    s = factor * jnp.concatenate([down_first_gradient, up_second_gradient], axis=1)
    s = jnp.pad(s.reshape(NDP, COLS), ((0, 0), (0, 1024 - COLS))).reshape(NDP, 8, 128)
    u_sum, s_sum = final_sums(u, s)
    u_sum = u_sum.reshape(ROWS, 2 * ADAPTER_RANK)
    s_sum = s_sum.reshape(1024)[:COLS].reshape(COLS // NDP, 2 * ADAPTER_RANK)
    return (
        u_sum[:, :ADAPTER_RANK],
        s_sum[:, ADAPTER_RANK:].T,
        s_sum[:, :ADAPTER_RANK],
        u_sum[:, ADAPTER_RANK:].T,
    )


def solution(mesh):
    return jax.shard_map(
        per_device,
        mesh=mesh,
        in_specs=(
            P("dp", "mp"),
            P("dp", "mp"),
            P("dp"),
            P(),
            P("dp", "mp"),
            P("dp", "mp"),
            P("dp", "mp"),
            P(),
            P(None, "mp"),
            P("mp", None),
            P(),
        ),
        out_specs=(P("dp", None), P(None, ("mp", "dp")), P(("mp", "dp"), None), P(None, "dp")),
        check_vma=False,
    )
```

```python
import math

import jax
import jax.numpy as jnp
from jax import lax
from jax.experimental import pallas as pl
from jax.experimental.pallas import tpu as pltpu
from jax.sharding import PartitionSpec as P

MODEL_WIDTH = 5120
HIDDEN_SHARD = 6912
ADAPTER_RANK = 16

norm_eps = 1e-06
adapter_scale = 2.0
clip_coefficient = 0.005

NZ, NY, NX, NC = 8, 4, 4, 2
NMP = NX * NC
NDP = NZ * NY
ROWS = 160
KLEN = ROWS * NZ
SEQ = 256
COLS = 864
WIDE = 896
HALF = ROWS // 2

PIECES = ((0, 0, 0, 896), (1, 0, 0, 896), (2, 1, 384, 512), (2, 1, 0, 384))
RING = (((0, 0), (0, 1), (1, 0), (1, 1), (2, 0), (2, 1), (3, 0)), ((0, 0), (0, 1), (1, 0), (1, 1), (2, 0), (2, 1), (3, 1)))
ORDER = (
    *((0, i) for i in range(7)), *((1, i) for i in range(7)),
    (2, 0), (2, 1), (2, 2), (2, 3), (3, 0), (3, 1), (2, 4), (2, 5), (3, 2), (3, 3), (2, 6), (3, 4), (3, 5), (3, 6),
)
LANE0 = 768
SPOT = COLS - LANE0
FEATS = MODEL_WIDTH // NMP
SHARE = COLS // NDP
MESH = pl.DeviceIdType.MESH
BF, F32 = jnp.bfloat16, jnp.float32


def contract_row_dims(left, right):
    return lax.dot_general(left, right, (((0,), (0,)), ((), ())), preferred_element_type=F32)


def contract_columns(left, right):
    return lax.dot_general(left, right, (((1,), (1,)), ((), ())), preferred_element_type=F32)


def remote(src, dst, send, recv, dp, mp):
    return pltpu.make_async_remote_copy(
        src_ref=src, dst_ref=dst, send_sem=send, recv_sem=recv, device_id={"dp": dp, "mp": mp}, device_id_type=MESH
    )


def signal(sem, dp, mp):
    pl.semaphore_signal(sem, inc=1, device_id={"dp": dp, "mp": mp}, device_id_type=MESH)


def gradients_kernel(
    lengths, xin, gin, gain, wg, wu, wd, adp, ad, u_out, s_out,
    c, at, wb, xt, a_all, b_all, cs2, cs1, near, cr2, cr1, ps, p_all, lat, hid, full, v, v_all, q, q_all, part, msg, msg_all, us, u_row,
    bs, br, ays, ayr, loc, axs, axr, ads, adr, c2s, c2r, c1s, c1r, pss, psr, vs, vr, qs, qr, ms, mr, us4, ur4,
):
    d, m = lax.axis_index("dp"), lax.axis_index("mp")
    z, y, x, core = d // NY, lax.rem(d, NY), m // NC, lax.rem(m, NC)

    def dp_of(zz, yy):
        return lax.rem(zz, NZ) * NY + lax.rem(yy, NY)

    def mp_of(xx, cc):
        return lax.rem(xx, NX) * NC + cc

    up_z, down_z = dp_of(z + 1, y), dp_of(z + NZ - 1, y)
    up_y, down_y = dp_of(z, y + 1), dp_of(z, y + NY - 1)
    up_x, down_x = mp_of(x + 1, core), mp_of(x + NX - 1, core)
    far_x = mp_of(x + 2, core)
    twin = mp_of(x, 1 - core)

    bar = pltpu.get_barrier_semaphore()
    signal(bar, up_z, m)
    signal(bar, down_z, m)
    for k in range(1, NY):
        signal(bar, dp_of(z, y + k), m)
    for k in range(1, NMP):
        signal(bar, d, lax.rem(m + k, NMP))

    def assemble(w, ref):
        wb[w, :, :COLS] = ref[...]
        tile = wb[w, :, LANE0:]
        lane = lax.broadcasted_iota(jnp.int32, tile.shape, 1)
        wb[w, :, LANE0:] = jnp.where(lane < SPOT, tile, adp[w])

    assemble(0, wg)
    pl.semaphore_wait(bar, 2 + NY - 1 + NMP - 1)

    def rows_of(zz, h, n):
        return pl.ds(pl.multiple_of(zz * ROWS + h * HALF, 16), n)

    def ring_copy(p, way, i):
        w, _, c0, n = PIECES[p]
        s, h = RING[way][i]
        src_z = lax.rem(z + (NZ - s if way == 0 else s), NZ)
        cols = pl.ds(c0, n)
        here = wb.at[w, pl.ds(h * HALF, HALF), cols] if s == 0 else b_all.at[w, rows_of(src_z, h, HALF), cols]
        there = b_all.at[w, rows_of(src_z, h, HALF), cols]
        return remote(here, there, bs.at[p, way, i], br.at[p, way, i], up_z if way == 0 else down_z, m)

    def ring_issue(p, i):
        for way in range(2):
            s, h = RING[way][i]
            if s:
                ring_copy(p, way, 2 * (s - 1) + h).wait_recv()
            ring_copy(p, way, i).start()

    def ring_finish(p):
        for way in range(2):
            for i in (5, 6) if way == 0 else (4, 6):
                ring_copy(p, way, i).wait_recv()

    def feats(mm):
        return pl.ds(pl.multiple_of(mm * ROWS, 16), ROWS)

    def y_copy(a, k):
        yy = lax.rem(y + k, NY)
        return remote(at.at[yy, a], a_all.at[y, a, feats(m), :], ays.at[a, k - 1], ayr.at[a, k - 1], dp_of(z, yy), m)

    def own_copy(a):
        return pltpu.make_async_copy(at.at[y, a], a_all.at[y, a, feats(m), :], loc.at[a])

    def block(a, mm, e0, ne):
        return a_all.at[pl.ds(e0, ne), a, feats(mm), :]

    def x_copy(a, i):
        mm, e0, ne, to = ((m, 0, 4, up_x), (m, 0, 4, down_x), (down_x, 0, 2, up_x), (up_x, 2, 2, down_x))[i]
        return remote(block(a, mm, e0, ne), block(a, mm, e0, ne), axs.at[a, i], axr.at[a, i], d, to)

    def core_copy(a, i):
        mm, e0, ne = ((m, 0, 4), (down_x, 0, 4), (up_x, 0, 4), (far_x, 0, 2), (far_x, 2, 2))[i]
        return remote(block(a, mm, e0, ne), block(a, mm, e0, ne), ads.at[a, i], adr.at[a, i], d, twin)

    def tokens_start(a):
        for k in (2, 1, 3):
            y_copy(a, k).start()
        own_copy(a).start()

    def tokens_x(a):
        own_copy(a).wait()
        for k in (1, 2, 3):
            y_copy(a, k).wait_recv()
        x_copy(a, 0).start()
        x_copy(a, 1).start()
        core_copy(a, 0).start()

    def tokens_on(a):
        x_copy(a, 0).wait_recv()
        x_copy(a, 2).start()
        x_copy(a, 1).wait_recv()
        x_copy(a, 3).start()
        core_copy(a, 1).start()
        core_copy(a, 2).start()

    def tokens_last(a):
        x_copy(a, 2).wait_recv()
        core_copy(a, 3).start()
        x_copy(a, 3).wait_recv()
        core_copy(a, 4).start()

    def tokens_done(a):
        for i in range(5):
            core_copy(a, i).wait_recv()

    def product(p, t, store):
        w, a, c0, n = PIECES[p]

        def tile(lo, size):
            acc = lax.dot_general(
                a_all[t, a], b_all[w, :, pl.ds(lo, size)], (((0,), (0,)), ((), ())), preferred_element_type=F32
            )
            store(w, lo, size, acc)

        def step(i, carry):
            tile(pl.multiple_of(c0 + i * 256, 128), 256)
            return carry

        lax.fori_loop(0, n // 256, step, 0)
        if n % 256:
            tile(c0 + n - n % 256, n % 256)

    def half_copy(p, way):
        w, _, c0, n = PIECES[p]
        cols = pl.ds(c0, n)
        return remote(
            cs2.at[w, way, :, cols], cr2.at[w, way, :, cols], c2s.at[p, way], c2r.at[p, way], up_y if way == 0 else down_y, m
        )

    def full_copy(p, way, h):
        w, _, c0, n = PIECES[p]
        part = (way, pl.ds(h * 128, 128), pl.ds(c0, n))
        return remote(
            cs1.at[(w, *part)], cr1.at[(w, *part)], c1s.at[p, way, h], c1r.at[p, way, h], up_y if way == 0 else down_y, m
        )

    def unit_far(p):
        def store(w, lo, size, acc):
            v = acc.astype(BF)
            cs2[w, 0, :, pl.ds(lo, size)] = v[:128]
            cs2[w, 1, :, pl.ds(lo, size)] = v[128:]

        product(p, lax.rem(y + 2, NY), store)
        half_copy(p, 0).start()
        half_copy(p, 1).start()

    def unit_near(p, way):
        def store(w, lo, size, acc):
            sent, kept = (acc[128:], acc[:128]) if way == 0 else (acc[:128], acc[128:])
            cs1[w, way, pl.ds((1 - way) * 128, 128), pl.ds(lo, size)] = sent.astype(BF)
            near[w, way, :, pl.ds(lo, size)] = kept

        product(p, lax.rem(y + (1 if way == 0 else NY - 1), NY), store)
        full_copy(p, way, 1 - way).start()

    def unit_pass(p):
        w, _, c0, n = PIECES[p]
        for way in range(2):
            half_copy(p, way).wait_recv()
            at_rows, cols = pl.ds(way * 128, 128), pl.ds(c0, n)
            total = near[w, way, :, cols] + cr2[w, way, :, cols].astype(F32)
            cs1[w, way, at_rows, cols] = total.astype(BF)
            full_copy(p, way, way).start()

    def unit_own(p):
        def store(w, lo, size, acc):
            c[w, :, pl.ds(lo, size)] = acc

        product(p, y, store)

    def unit_sum(p):
        w, _, c0, n = PIECES[p]
        cols = pl.ds(c0, n)
        for way in range(2):
            for h in range(2):
                full_copy(p, way, h).wait_recv()
        c[w, :, cols] += cr1[w, 0, :, cols].astype(F32) + cr1[w, 1, :, cols].astype(F32)

    def p_copy(k):
        return remote(ps, p_all.at[m], pss.at[k - 1], psr.at[k - 1], d, lax.rem(m + k, NMP))

    def own_rows():
        for w in range(3):
            b_all[w, rows_of(z, 0, ROWS), :] = wb[w]

    def normalize():
        p_all[m] = ps[...]
        for k in range(1, NMP):
            p_copy(k).wait_recv()
        inverse = lax.rsqrt(jnp.sum(p_all[...], axis=0)[:1] * (1.0 / MODEL_WIDTH) + norm_eps)
        gains = gain[...].astype(F32).T
        lane = lax.broadcasted_iota(jnp.int32, gains.shape, 1)
        column = jnp.sum(jnp.where(lane == m, gains, 0.0), axis=1, keepdims=True)
        normed = (xt[...] * inverse * column).astype(BF)
        for yy in range(NY):
            at[yy, 0] = normed[yy * ROWS : (yy + 1) * ROWS]

    def mask():
        token = lax.broadcasted_iota(jnp.int32, (1, SEQ), 1)
        live = (token < lengths[0]).astype(F32)
        masked = (gin[...].astype(F32).T * live).astype(BF)
        for yy in range(NY):
            at[yy, 1] = masked[yy * ROWS : (yy + 1) * ROWS]

    def rest():
        xt[...] = xin[...].astype(F32).T
        ps[...] = jnp.broadcast_to(jnp.sum(xt[...] * xt[...], axis=0, keepdims=True), ps.shape)
        for k in range(1, NMP):
            p_copy(k).start()
        assemble(1, wu)
        normalize()
        tokens_start(0)
        mask()
        tokens_start(1)
        assemble(2, wd)
        own_rows()

    def tile_of(i):
        return pl.ds(pl.multiple_of(i * 128, 128), 128)

    def spots(a):
        return a[SPOT : SPOT + ADAPTER_RANK]

    def forward_side():
        up_latent = c[1, :, LANE0:].astype(BF)
        lat[...] = jnp.zeros_like(lat)

        def chunk(i, carry):
            cols = tile_of(i)
            gate_act = jax.nn.silu(c[0, :, cols])
            c[0, :, cols] = gate_act
            up = c[1, :, cols] + adapter_scale * jnp.dot(up_latent, ad[0, :, cols], preferred_element_type=F32)
            hidden = (gate_act * up).astype(BF)
            hid[:, cols] = hidden
            lat[0] += contract_columns(ad[1, :, cols], hidden)
            return carry

        lax.fori_loop(0, WIDE // 128, chunk, 0)
        v[0] = spots(lat[0]).astype(BF)
        for k in range(1, NMP):
            v_copy(0, k).start()

    def down_side():
        v_all[0, m] = v[0]
        for k in range(1, NMP):
            v_copy(0, k).wait_recv()
        latent = jnp.sum(v_all[0].astype(F32), axis=0).astype(BF)
        for yy in range(NY):
            put(yy, 4, adapter_scale * contract_columns(latent, at[yy, 1]))

    def backward_side(lo, hi):
        up_latent = c[1, :, LANE0:].astype(BF)
        back_latent = c[2, :, LANE0:].astype(BF)

        def chunk(i, carry):
            cols = tile_of(i)
            back = c[2, :, cols] + adapter_scale * jnp.dot(back_latent, ad[1, :, cols], preferred_element_type=F32)
            up_gradient = (back * c[0, :, cols]).astype(BF)
            lat[1] += contract_columns(ad[0, :, cols], up_gradient)
            full[:ADAPTER_RANK, cols] = adapter_scale * spots(contract_row_dims(back_latent, hid[:, cols]))
            full[ADAPTER_RANK:, cols] = adapter_scale * spots(contract_row_dims(up_latent, up_gradient))
            return carry

        lax.fori_loop(lo, hi, chunk, 0)

    def v_copy(i, k):
        return remote(v.at[i], v_all.at[i, m], vs.at[i, k - 1], vr.at[i, k - 1], d, lax.rem(m + k, NMP))

    def q_copy(k):
        return remote(q, q_all.at[m], qs.at[k - 1], qr.at[k - 1], d, lax.rem(m + k, NMP))

    def put(yy, j0, rows):
        for j in range(4):
            part[(j0 + j) * NY + yy, 8:12] = rows[4 * j : 4 * j + 4, :128]
            part[(j0 + j) * NY + yy, 12:16, : ROWS - 128] = rows[4 * j : 4 * j + 4, 128:]

    plan = {
        1: [rest],
        3: [lambda: tokens_x(0)],
        6: [lambda: tokens_on(0), lambda: tokens_x(1)],
        8: [lambda: tokens_last(0)],
        9: [lambda: ring_finish(0), lambda: tokens_done(0), lambda: unit_far(0)],
        10: [lambda: unit_near(0, 0)],
        11: [lambda: unit_near(0, 1)],
        12: [lambda: tokens_on(1), lambda: unit_pass(0)],
        13: [lambda: unit_own(0)],
        15: [lambda: tokens_last(1)],
        16: [lambda: ring_finish(1), lambda: unit_far(1)],
        17: [lambda: unit_near(1, 0)],
        18: [lambda: unit_near(1, 1)],
        19: [lambda: unit_sum(0)],
        20: [lambda: unit_pass(1)],
        21: [lambda: unit_own(1), lambda: tokens_done(1)],
        27: [lambda: ring_finish(2), lambda: unit_far(2), lambda: unit_near(2, 0), lambda: unit_near(2, 1)],
    }
    part[...] = jnp.zeros_like(part)
    for at_position, (p, i) in enumerate(ORDER):
        ring_issue(p, i)
        for u in plan.get(at_position, ()):
            u()
    ring_finish(3)
    unit_far(3)
    unit_near(3, 0)
    unit_near(3, 1)
    unit_pass(2)
    unit_own(2)
    unit_sum(1)
    forward_side()
    unit_pass(3)
    unit_own(3)
    down_side()
    unit_sum(2)
    backward_side(3, WIDE // 128)
    unit_sum(3)
    backward_side(0, 3)
    v[1] = spots(lat[1]).astype(BF)
    for k in range(1, NMP):
        v_copy(1, k).start()
    v_all[1, m] = v[1]

    for i in range(NDP):
        for r in range(4):
            part[i, :8, r * 32 : r * 32 + 32] = full[r * 8 : r * 8 + 8, i * SHARE : i * SHARE + 32]
    squares = jnp.sum(full[...] * full[...], keepdims=True)
    for k in range(1, NMP):
        v_copy(1, k).wait_recv()
    latent = jnp.sum(v_all[1].astype(F32), axis=0).astype(BF)
    for yy in range(NY):
        put(yy, 0, adapter_scale * contract_columns(latent, at[yy, 0]))
    features = part[:, 8:, :]
    squares = squares + jnp.sum(jnp.sum(features * features, axis=0), keepdims=True)
    q[...] = jnp.broadcast_to(squares, q.shape)
    for k in range(1, NMP):
        q_copy(k).start()
    q_all[m] = q[...]
    for k in range(1, NMP):
        q_copy(k).wait_recv()
    clip_limit = clip_coefficient * math.sqrt(2.0 * ADAPTER_RANK * (MODEL_WIDTH + HIDDEN_SHARD))
    norm = jnp.sqrt(jnp.sum(q_all[...], axis=0))
    factor = jnp.minimum(1.0, clip_limit / (norm + 1e-06))[:1, :1]
    msg[...] = (part[...] * factor[None]).astype(BF)

    def m_copy(k):
        dd = lax.rem(d + k, NDP)
        return remote(msg.at[dd], msg_all.at[d], ms.at[k], mr.at[d], dd, m)

    def m_start(k, carry):
        m_copy(k).start()
        return carry

    def m_arrive(k, carry):
        dd = lax.rem(d + k, NDP)
        remote(msg.at[0], msg_all.at[dd], ms.at[k], mr.at[dd], dd, m).wait_recv()
        return carry

    lax.fori_loop(1, NDP, m_start, 0)
    msg_all[d] = msg[d]
    lax.fori_loop(1, NDP, m_arrive, 0)
    summed = jnp.sum(msg_all[...].astype(F32), axis=0)
    us[...] = summed[8:]

    goal = m * NY + y
    here = z == m

    def u_copy(k):
        return remote(us, u_row.at[z], us4.at[k], ur4.at[z], goal, lax.rem(m + k, NMP))

    for k in range(1, NMP):
        u_copy(k).start()

    @pl.when(jnp.logical_not(here))
    def _():
        u_copy(0).start()

    @pl.when(here)
    def _():
        u_row[z] = us[...]

    for r in range(4):
        s_out[r * 8 : r * 8 + 8] = summed[:8, r * 32 : r * 32 + SHARE]

    for j in range(NZ):
        @pl.when(jnp.logical_not(jnp.logical_and(here, z == j)))
        def _():
            remote(us, u_row.at[j], us4.at[0], ur4.at[j], goal, lax.rem(m + 1, NMP)).wait_recv()

        u_out[4 * j : 4 * j + 4, :128] = u_row[j, :4]
        u_out[4 * j : 4 * j + 4, 128:] = u_row[j, 4:, : ROWS - 128]

    def m_sent(k, carry):
        m_copy(k).wait_send()
        return carry

    lax.fori_loop(1, NDP, m_sent, 0)
    for k in range(1, NMP):
        v_copy(0, k).wait_send()
        v_copy(1, k).wait_send()
        q_copy(k).wait_send()
        u_copy(k).wait_send()

    @pl.when(jnp.logical_not(here))
    def _():
        u_copy(0).wait_send()

    for p in range(4):
        for way in range(2):
            for i in range(7):
                ring_copy(p, way, i).wait_send()
            half_copy(p, way).wait_send()
            for h in range(2):
                full_copy(p, way, h).wait_send()
    for a in range(2):
        for k in (1, 2, 3):
            y_copy(a, k).wait_send()
        for i in range(4):
            x_copy(a, i).wait_send()
        for i in range(5):
            core_copy(a, i).wait_send()
    for k in range(1, NMP):
        p_copy(k).wait_send()


def gradients(lengths, x, g, gain, wg, wu, wd, adp, ad):
    vmem = pl.BlockSpec(memory_space=pltpu.VMEM)
    dma = pltpu.SemaphoreType.DMA
    return pl.pallas_call(
        gradients_kernel,
        out_shape=(
            jax.ShapeDtypeStruct((2 * ADAPTER_RANK, ROWS), F32),
            jax.ShapeDtypeStruct((2 * ADAPTER_RANK, SHARE), F32),
        ),
        in_specs=[pl.BlockSpec(memory_space=pltpu.SMEM), *[vmem] * 8],
        out_specs=(vmem, vmem),
        scratch_shapes=[
            pltpu.VMEM((3, SEQ, WIDE), F32),
            pltpu.VMEM((NY, 2, ROWS, SEQ), BF),
            pltpu.VMEM((3, ROWS, WIDE), BF),
            pltpu.VMEM((FEATS, SEQ), F32),
            pltpu.VMEM((NY, 2, KLEN, SEQ), BF),
            pltpu.VMEM((3, KLEN, WIDE), BF),
            pltpu.VMEM((3, 2, 128, WIDE), BF),
            pltpu.VMEM((3, 2, SEQ, WIDE), BF),
            pltpu.VMEM((3, 2, 128, WIDE), F32),
            pltpu.VMEM((3, 2, 128, WIDE), BF),
            pltpu.VMEM((3, 2, SEQ, WIDE), BF),
            pltpu.VMEM((8, SEQ), F32),
            pltpu.VMEM((NMP, 8, SEQ), F32),
            pltpu.VMEM((2, 128, SEQ), F32),
            pltpu.VMEM((SEQ, WIDE), BF),
            pltpu.VMEM((2 * ADAPTER_RANK, WIDE), F32),
            pltpu.VMEM((2, ADAPTER_RANK, SEQ), BF),
            pltpu.VMEM((2, NMP, ADAPTER_RANK, SEQ), BF),
            pltpu.VMEM((8, 128), F32),
            pltpu.VMEM((NMP, 8, 128), F32),
            pltpu.VMEM((NDP, 16, 128), F32),
            pltpu.VMEM((NDP, 16, 128), BF),
            pltpu.VMEM((NDP, 16, 128), BF),
            pltpu.VMEM((8, 128), F32),
            pltpu.VMEM((NZ, 8, 128), F32),
            dma((4, 2, 7)),
            dma((4, 2, 7)),
            dma((2, 3)),
            dma((2, 3)),
            dma((2,)),
            dma((2, 4)),
            dma((2, 4)),
            dma((2, 5)),
            dma((2, 5)),
            dma((4, 2)),
            dma((4, 2)),
            dma((4, 2, 2)),
            dma((4, 2, 2)),
            dma((NMP - 1,)),
            dma((NMP - 1,)),
            dma((2, NMP - 1)),
            dma((2, NMP - 1)),
            dma((NMP - 1,)),
            dma((NMP - 1,)),
            dma((NDP,)),
            dma((NDP,)),
            dma((NMP,)),
            dma((NMP,)),
        ],
        compiler_params=pltpu.CompilerParams(collective_id=0, has_side_effects=True),
        name="gradients",
    )(lengths, x, g, gain, wg, wu, wd, adp, ad)


def per_device(
    residual_input,
    cotangent,
    lengths,
    norm_gain_vector,
    gate_projection_weight,
    up_projection_weight,
    down_projection_weight,
    up_adapter_first,
    up_adapter_second,
    down_adapter_first,
    down_adapter_second,
):
    d = lax.axis_index("dp")
    first = lax.dynamic_slice(up_adapter_first, (d * ROWS, 0), (ROWS, ADAPTER_RANK))
    second = lax.dynamic_slice(down_adapter_second, (0, d * ROWS), (ADAPTER_RANK, ROWS)).T
    adp = jnp.stack([jnp.zeros_like(first), first, second])
    adp = jnp.pad(adp, ((0, 0), (0, 0), (SPOT, 128 - SPOT - ADAPTER_RANK)))
    ad = jnp.stack([up_adapter_second, down_adapter_first.T])
    ad = jnp.pad(ad, ((0, 0), (SPOT, 128 - SPOT - ADAPTER_RANK), (0, WIDE - COLS)))
    u, s = gradients(
        lengths,
        residual_input,
        cotangent,
        norm_gain_vector.reshape(NMP, FEATS),
        gate_projection_weight,
        up_projection_weight,
        down_projection_weight,
        adp,
        ad,
    )
    return (u[:ADAPTER_RANK].T, s[ADAPTER_RANK:], s[:ADAPTER_RANK].T, u[ADAPTER_RANK:])


def solution(mesh):
    return jax.shard_map(
        per_device,
        mesh=mesh,
        in_specs=(
            P("dp", "mp"),
            P("dp", "mp"),
            P("dp"),
            P(),
            P("dp", "mp"),
            P("dp", "mp"),
            P("dp", "mp"),
            P(),
            P(None, "mp"),
            P("mp", None),
            P(),
        ),
        out_specs=(P("dp", None), P(None, ("mp", "dp")), P(("mp", "dp"), None), P(None, "dp")),
        check_vma=False,
    )
```

```python
import math

import jax
import jax.numpy as jnp
from jax import lax
from jax.experimental import pallas as pl
from jax.experimental.pallas import tpu as pltpu
from jax.sharding import PartitionSpec as P

MODEL_WIDTH = 5120
HIDDEN_SHARD = 6912
ADAPTER_RANK = 16

norm_eps = 1e-06
adapter_scale = 2.0
clip_coefficient = 0.005

NZ, NY, NX, NC = 8, 4, 4, 2
NMP = NX * NC
NDP = NZ * NY
ROWS = 160
KLEN = ROWS * NZ
SEQ = 256
COLS = 864
WIDE = 896
HALF = ROWS // 2

PIECES = ((0, 0, 0, 896), (1, 0, 0, 896), (2, 1, 384, 512), (2, 1, 0, 384))
RING = (((0, 0), (0, 1), (1, 0), (1, 1), (2, 0), (2, 1), (3, 0)), ((0, 0), (0, 1), (1, 0), (1, 1), (2, 0), (2, 1), (3, 1)))
ORDER = (
    *((0, i) for i in range(7)), *((1, i) for i in range(6)),
    (2, 0), (2, 1), (1, 6), (2, 2), (2, 3), (2, 4), (2, 5), (3, 0), (3, 1), (2, 6), (3, 2), (3, 3), (3, 4), (3, 5), (3, 6),
)
LANE0 = 768
SPOT = COLS - LANE0
FEATS = MODEL_WIDTH // NMP
SHARE = COLS // NDP
MESH = pl.DeviceIdType.MESH
BF, F32 = jnp.bfloat16, jnp.float32


def contract_row_dims(left, right):
    return lax.dot_general(left, right, (((0,), (0,)), ((), ())), preferred_element_type=F32)


def contract_columns(left, right):
    return lax.dot_general(left, right, (((1,), (1,)), ((), ())), preferred_element_type=F32)


def remote(src, dst, send, recv, dp, mp):
    return pltpu.make_async_remote_copy(
        src_ref=src, dst_ref=dst, send_sem=send, recv_sem=recv, device_id={"dp": dp, "mp": mp}, device_id_type=MESH
    )


def signal(sem, dp, mp):
    pl.semaphore_signal(sem, inc=1, device_id={"dp": dp, "mp": mp}, device_id_type=MESH)


def gradients_kernel(
    lengths, x_in, g_in, w0_in, w1_in, w2_in, up_a, down_b, gain, up_b, down_a, up_a_out, up_b_out, down_a_out, down_b_out,
    xin, gin, win, window, turn, ad, lsem, c, at, wb, xt, a_all, b_all, cs2, cs1, near, cr2, cr1, ps, p_all, lat, hid, full, v, v_all, q, q_all, part, msg, msg_all, us, u_row,
    bs, br, ays, ayr, loc, axs, axr, ads, adr, c2s, c2r, c1s, c1r, pss, psr, vs, vr, qs, qr, ms, mr, us4, ur4,
):
    d, m = lax.axis_index("dp"), lax.axis_index("mp")
    z, y, x, core = d // NY, lax.rem(d, NY), m // NC, lax.rem(m, NC)

    def dp_of(zz, yy):
        return lax.rem(zz, NZ) * NY + lax.rem(yy, NY)

    def mp_of(xx, cc):
        return lax.rem(xx, NX) * NC + cc

    up_z, down_z = dp_of(z + 1, y), dp_of(z + NZ - 1, y)
    up_y, down_y = dp_of(z, y + 1), dp_of(z, y + NY - 1)
    up_x, down_x = mp_of(x + 1, core), mp_of(x + NX - 1, core)
    far_x = mp_of(x + 2, core)
    twin = mp_of(x, 1 - core)

    bar = pltpu.get_barrier_semaphore()
    signal(bar, up_z, m)
    signal(bar, down_z, m)
    for k in range(1, NY):
        signal(bar, dp_of(z, y + k), m)
    for k in range(1, NMP):
        signal(bar, d, lax.rem(m + k, NMP))

    lanes = pl.ds(pl.multiple_of(d * (ROWS // 32) // 4 * 128, 128), SEQ)
    loads = (
        (w0_in, win.at[0]),
        (x_in, xin),
        (w1_in, win.at[1]),
        (g_in, gin),
        (w2_in, win.at[2]),
        (up_a.at[:, lanes], window.at[0]),
        (down_b.at[:, lanes], window.at[1]),
    )

    def load(i):
        return pltpu.make_async_copy(*loads[i], lsem.at[i])

    for i in range(len(loads)):
        load(i).start()

    def adapter_rows(i):
        wide = window[i].astype(F32)
        rows = jnp.zeros((ADAPTER_RANK, ROWS), F32)
        for k in range(NY):
            rows = rows + jnp.where(y == k, wide[:, 32 * k : 32 * k + ROWS], 0.0)
        turn[...] = jnp.zeros_like(turn)
        turn[SPOT : SPOT + ADAPTER_RANK, :ROWS] = rows
        return turn[...].T[:ROWS].astype(BF)

    def assemble(w, beside):
        wb[w, :, :COLS] = win[w]
        tile = wb[w, :, LANE0:]
        lane = lax.broadcasted_iota(jnp.int32, tile.shape, 1)
        wb[w, :, LANE0:] = jnp.where(lane < SPOT, tile, beside)

    load(0).wait()
    assemble(0, jnp.zeros((ROWS, 128), BF))
    pl.semaphore_wait(bar, 2 + NY - 1 + NMP - 1)

    def rows_of(zz, h, n):
        return pl.ds(pl.multiple_of(zz * ROWS + h * HALF, 16), n)

    def ring_copy(p, way, i):
        w, _, c0, n = PIECES[p]
        s, h = RING[way][i]
        src_z = lax.rem(z + (NZ - s if way == 0 else s), NZ)
        cols = pl.ds(c0, n)
        here = wb.at[w, pl.ds(h * HALF, HALF), cols] if s == 0 else b_all.at[w, rows_of(src_z, h, HALF), cols]
        there = b_all.at[w, rows_of(src_z, h, HALF), cols]
        return remote(here, there, bs.at[p, way, i], br.at[p, way, i], up_z if way == 0 else down_z, m)

    def ring_issue(p, i):
        for way in range(2):
            s, h = RING[way][i]
            if s:
                ring_copy(p, way, 2 * (s - 1) + h).wait_recv()
            ring_copy(p, way, i).start()

    def ring_finish(p):
        for way in range(2):
            for i in (5, 6) if way == 0 else (4, 6):
                ring_copy(p, way, i).wait_recv()

    def feats(mm):
        return pl.ds(pl.multiple_of(mm * ROWS, 16), ROWS)

    def y_copy(a, k):
        yy = lax.rem(y + k, NY)
        return remote(at.at[yy, a], a_all.at[y, a, feats(m), :], ays.at[a, k - 1], ayr.at[a, k - 1], dp_of(z, yy), m)

    def own_copy(a):
        return pltpu.make_async_copy(at.at[y, a], a_all.at[y, a, feats(m), :], loc.at[a])

    def block(a, mm, e0, ne):
        return a_all.at[pl.ds(e0, ne), a, feats(mm), :]

    def x_copy(a, i):
        mm, e0, ne, to = ((m, 0, 4, up_x), (m, 0, 4, down_x), (down_x, 0, 2, up_x), (up_x, 2, 2, down_x))[i]
        return remote(block(a, mm, e0, ne), block(a, mm, e0, ne), axs.at[a, i], axr.at[a, i], d, to)

    def core_copy(a, i):
        mm, e0, ne = ((m, 0, 4), (down_x, 0, 4), (up_x, 0, 4), (far_x, 0, 2), (far_x, 2, 2))[i]
        return remote(block(a, mm, e0, ne), block(a, mm, e0, ne), ads.at[a, i], adr.at[a, i], d, twin)

    def tokens_start(a):
        for k in (2, 1, 3):
            y_copy(a, k).start()
        own_copy(a).start()

    def tokens_x(a):
        own_copy(a).wait()
        for k in (1, 2, 3):
            y_copy(a, k).wait_recv()
        x_copy(a, 0).start()
        x_copy(a, 1).start()
        core_copy(a, 0).start()

    def tokens_on(a):
        x_copy(a, 0).wait_recv()
        x_copy(a, 2).start()
        x_copy(a, 1).wait_recv()
        x_copy(a, 3).start()
        core_copy(a, 1).start()
        core_copy(a, 2).start()

    def tokens_last(a):
        x_copy(a, 2).wait_recv()
        core_copy(a, 3).start()
        x_copy(a, 3).wait_recv()
        core_copy(a, 4).start()

    def tokens_done(a):
        for i in range(5):
            core_copy(a, i).wait_recv()

    def product(p, t, store):
        w, a, c0, n = PIECES[p]

        def tile(lo, size):
            acc = lax.dot_general(
                a_all[t, a], b_all[w, :, pl.ds(lo, size)], (((0,), (0,)), ((), ())), preferred_element_type=F32
            )
            store(w, lo, size, acc)

        def step(i, carry):
            tile(pl.multiple_of(c0 + i * 256, 128), 256)
            return carry

        lax.fori_loop(0, n // 256, step, 0)
        if n % 256:
            tile(c0 + n - n % 256, n % 256)

    def half_copy(p, way):
        w, _, c0, n = PIECES[p]
        cols = pl.ds(c0, n)
        return remote(
            cs2.at[w, way, :, cols], cr2.at[w, way, :, cols], c2s.at[p, way], c2r.at[p, way], up_y if way == 0 else down_y, m
        )

    def full_copy(p, way, h):
        w, _, c0, n = PIECES[p]
        part = (way, pl.ds(h * 128, 128), pl.ds(c0, n))
        return remote(
            cs1.at[(w, *part)], cr1.at[(w, *part)], c1s.at[p, way, h], c1r.at[p, way, h], up_y if way == 0 else down_y, m
        )

    def unit_far(p):
        def store(w, lo, size, acc):
            v = acc.astype(BF)
            cs2[w, 0, :, pl.ds(lo, size)] = v[:128]
            cs2[w, 1, :, pl.ds(lo, size)] = v[128:]

        product(p, lax.rem(y + 2, NY), store)
        half_copy(p, 0).start()
        half_copy(p, 1).start()

    def unit_near(p, way):
        def store(w, lo, size, acc):
            sent, kept = (acc[128:], acc[:128]) if way == 0 else (acc[:128], acc[128:])
            cs1[w, way, pl.ds((1 - way) * 128, 128), pl.ds(lo, size)] = sent.astype(BF)
            near[w, way, :, pl.ds(lo, size)] = kept

        product(p, lax.rem(y + (1 if way == 0 else NY - 1), NY), store)
        full_copy(p, way, 1 - way).start()

    def unit_pass(p):
        w, _, c0, n = PIECES[p]
        for way in range(2):
            half_copy(p, way).wait_recv()
            at_rows, cols = pl.ds(way * 128, 128), pl.ds(c0, n)
            total = near[w, way, :, cols] + cr2[w, way, :, cols].astype(F32)
            cs1[w, way, at_rows, cols] = total.astype(BF)
            full_copy(p, way, way).start()

    def unit_own(p):
        def store(w, lo, size, acc):
            c[w, :, pl.ds(lo, size)] = acc

        product(p, y, store)

    def unit_sum(p):
        w, _, c0, n = PIECES[p]
        cols = pl.ds(c0, n)
        for way in range(2):
            for h in range(2):
                full_copy(p, way, h).wait_recv()
        c[w, :, cols] += cr1[w, 0, :, cols].astype(F32) + cr1[w, 1, :, cols].astype(F32)

    def p_copy(k):
        return remote(ps, p_all.at[m], pss.at[k - 1], psr.at[k - 1], d, lax.rem(m + k, NMP))

    def own_rows():
        for w in range(3):
            b_all[w, rows_of(z, 0, ROWS), :] = wb[w]

    def normalize():
        p_all[m] = ps[...]
        for k in range(1, NMP):
            p_copy(k).wait_recv()
        inverse = lax.rsqrt(jnp.sum(p_all[...], axis=0)[:1] * (1.0 / MODEL_WIDTH) + norm_eps)
        gains = gain[...].astype(F32).T
        lane = lax.broadcasted_iota(jnp.int32, gains.shape, 1)
        column = jnp.concatenate(
            [
                jnp.sum(jnp.where(lane == m * (FEATS // 128) + i, gains, 0.0), axis=1, keepdims=True)
                for i in range(FEATS // 128)
            ],
            axis=0,
        )
        normed = (xt[...] * inverse * column).astype(BF)
        for yy in range(NY):
            at[yy, 0] = normed[yy * ROWS : (yy + 1) * ROWS]

    def mask():
        token = lax.broadcasted_iota(jnp.int32, (1, SEQ), 1)
        live = (token < lengths[0]).astype(F32)
        masked = (gin[...].astype(F32).T * live).astype(BF)
        for yy in range(NY):
            at[yy, 1] = masked[yy * ROWS : (yy + 1) * ROWS]

    def rest():
        load(1).wait()
        xt[...] = xin[...].astype(F32).T
        ps[...] = jnp.broadcast_to(jnp.sum(xt[...] * xt[...], axis=0, keepdims=True), ps.shape)
        for k in range(1, NMP):
            p_copy(k).start()
        load(2).wait()
        load(5).wait()
        assemble(1, adapter_rows(0))
        normalize()
        tokens_start(0)
        load(3).wait()
        mask()
        tokens_start(1)
        load(4).wait()
        load(6).wait()
        assemble(2, adapter_rows(1))
        own_rows()
        part[...] = jnp.zeros_like(part)
        ad[...] = jnp.zeros_like(ad)
        ad[0, SPOT : SPOT + ADAPTER_RANK, :COLS] = up_b[...]
        ad[1, SPOT : SPOT + ADAPTER_RANK, :COLS] = down_a[...]

    def tile_of(i):
        return pl.ds(pl.multiple_of(i * 128, 128), 128)

    def spots(a):
        return a[SPOT : SPOT + ADAPTER_RANK]

    def forward_side():
        up_latent = c[1, :, LANE0:].astype(BF)
        lat[...] = jnp.zeros_like(lat)

        def chunk(i, carry):
            cols = tile_of(i)
            gate_act = jax.nn.silu(c[0, :, cols])
            c[0, :, cols] = gate_act
            up = c[1, :, cols] + adapter_scale * jnp.dot(up_latent, ad[0, :, cols], preferred_element_type=F32)
            hidden = (gate_act * up).astype(BF)
            hid[:, cols] = hidden
            lat[0] += contract_columns(ad[1, :, cols], hidden)
            return carry

        lax.fori_loop(0, WIDE // 128, chunk, 0)
        v[0] = spots(lat[0]).astype(BF)
        for k in range(1, NMP):
            v_copy(0, k).start()

    def down_side():
        v_all[0, m] = v[0]
        for k in range(1, NMP):
            v_copy(0, k).wait_recv()
        latent = jnp.sum(v_all[0].astype(F32), axis=0).astype(BF)
        for yy in range(NY):
            put(yy, 4, adapter_scale * contract_columns(latent, at[yy, 1]))

    def backward_side(lo, hi):
        up_latent = c[1, :, LANE0:].astype(BF)
        back_latent = c[2, :, LANE0:].astype(BF)

        def chunk(i, carry):
            cols = tile_of(i)
            back = c[2, :, cols] + adapter_scale * jnp.dot(back_latent, ad[1, :, cols], preferred_element_type=F32)
            up_gradient = (back * c[0, :, cols]).astype(BF)
            lat[1] += contract_columns(ad[0, :, cols], up_gradient)
            full[:ADAPTER_RANK, cols] = adapter_scale * spots(contract_row_dims(back_latent, hid[:, cols]))
            full[ADAPTER_RANK:, cols] = adapter_scale * spots(contract_row_dims(up_latent, up_gradient))
            return carry

        lax.fori_loop(lo, hi, chunk, 0)

    def v_copy(i, k):
        return remote(v.at[i], v_all.at[i, m], vs.at[i, k - 1], vr.at[i, k - 1], d, lax.rem(m + k, NMP))

    def q_copy(k):
        return remote(q, q_all.at[m], qs.at[k - 1], qr.at[k - 1], d, lax.rem(m + k, NMP))

    def put(yy, j0, rows):
        for j in range(4):
            part[(j0 + j) * NY + yy, 8:12] = rows[4 * j : 4 * j + 4, :128]
            part[(j0 + j) * NY + yy, 12:16, : ROWS - 128] = rows[4 * j : 4 * j + 4, 128:]

    plan = {
        1: [rest],
        3: [lambda: tokens_x(0)],
        6: [lambda: tokens_on(0), lambda: tokens_x(1)],
        8: [lambda: tokens_last(0)],
        9: [lambda: ring_finish(0), lambda: tokens_done(0), lambda: unit_far(0)],
        10: [lambda: unit_near(0, 0)],
        11: [lambda: unit_near(0, 1)],
        12: [lambda: tokens_on(1), lambda: unit_pass(0)],
        13: [lambda: unit_own(0)],
        14: [lambda: tokens_last(1)],
        18: [lambda: ring_finish(1), lambda: unit_far(1)],
        19: [lambda: unit_near(1, 0)],
        20: [lambda: unit_near(1, 1)],
        21: [lambda: unit_sum(0)],
        22: [lambda: unit_pass(1)],
        23: [lambda: unit_own(1), lambda: tokens_done(1)],
        25: [lambda: ring_finish(2), lambda: unit_far(2)],
        26: [lambda: unit_near(2, 0)],
        27: [lambda: unit_near(2, 1)],
    }
    for at_position, (p, i) in enumerate(ORDER):
        ring_issue(p, i)
        for u in plan.get(at_position, ()):
            u()
    ring_finish(3)
    unit_far(3)
    unit_near(3, 0)
    unit_near(3, 1)
    unit_pass(2)
    unit_own(2)
    unit_sum(1)
    forward_side()
    unit_pass(3)
    unit_own(3)
    down_side()
    unit_sum(2)
    backward_side(3, WIDE // 128)
    unit_sum(3)
    backward_side(0, 3)
    v[1] = spots(lat[1]).astype(BF)
    for k in range(1, NMP):
        v_copy(1, k).start()
    v_all[1, m] = v[1]

    for i in range(NDP):
        for r in range(4):
            part[i, :8, r * 32 : r * 32 + 32] = full[r * 8 : r * 8 + 8, i * SHARE : i * SHARE + 32]
    squares = jnp.sum(full[...] * full[...], keepdims=True)
    for k in range(1, NMP):
        v_copy(1, k).wait_recv()
    latent = jnp.sum(v_all[1].astype(F32), axis=0).astype(BF)
    for yy in range(NY):
        put(yy, 0, adapter_scale * contract_columns(latent, at[yy, 0]))
    features = part[:, 8:, :]
    squares = squares + jnp.sum(jnp.sum(features * features, axis=0), keepdims=True)
    q[...] = jnp.broadcast_to(squares, q.shape)
    for k in range(1, NMP):
        q_copy(k).start()
    q_all[m] = q[...]
    for k in range(1, NMP):
        q_copy(k).wait_recv()
    clip_limit = clip_coefficient * math.sqrt(2.0 * ADAPTER_RANK * (MODEL_WIDTH + HIDDEN_SHARD))
    norm = jnp.sqrt(jnp.sum(q_all[...], axis=0))
    factor = jnp.minimum(1.0, clip_limit / (norm + 1e-06))[:1, :1]
    msg[...] = (part[...] * factor[None]).astype(BF)

    def m_copy(k):
        dd = lax.rem(d + k, NDP)
        return remote(msg.at[dd], msg_all.at[d], ms.at[k], mr.at[d], dd, m)

    def m_start(k, carry):
        m_copy(k).start()
        return carry

    def m_arrive(k, carry):
        dd = lax.rem(d + k, NDP)
        remote(msg.at[0], msg_all.at[dd], ms.at[k], mr.at[dd], dd, m).wait_recv()
        return carry

    lax.fori_loop(1, NDP, m_start, 0)
    msg_all[d] = msg[d]
    lax.fori_loop(1, NDP, m_arrive, 0)
    summed = jnp.sum(msg_all[...].astype(F32), axis=0)
    us[...] = summed[8:]

    goal = m * NY + y
    here = z == m

    def u_copy(k):
        return remote(us, u_row.at[z], us4.at[k], ur4.at[z], goal, lax.rem(m + k, NMP))

    for k in range(1, NMP):
        u_copy(k).start()

    @pl.when(jnp.logical_not(here))
    def _():
        u_copy(0).start()

    @pl.when(here)
    def _():
        u_row[z] = us[...]

    for r in range(4):
        part_out = (down_a_out, up_b_out)[r // 2]
        part_out[r % 2 * 8 : r % 2 * 8 + 8] = summed[:8, r * 32 : r * 32 + SHARE]

    for j in range(NZ):
        @pl.when(jnp.logical_not(jnp.logical_and(here, z == j)))
        def _():
            remote(us, u_row.at[j], us4.at[0], ur4.at[j], goal, lax.rem(m + 1, NMP)).wait_recv()

        u_out = (up_a_out, down_b_out)[j // 4]
        u_out[j % 4 * 4 : j % 4 * 4 + 4, :128] = u_row[j, :4]
        u_out[j % 4 * 4 : j % 4 * 4 + 4, 128:] = u_row[j, 4:, : ROWS - 128]

    def m_sent(k, carry):
        m_copy(k).wait_send()
        return carry

    lax.fori_loop(1, NDP, m_sent, 0)
    for k in range(1, NMP):
        v_copy(0, k).wait_send()
        v_copy(1, k).wait_send()
        q_copy(k).wait_send()
        u_copy(k).wait_send()

    @pl.when(jnp.logical_not(here))
    def _():
        u_copy(0).wait_send()

    for p in range(4):
        for way in range(2):
            for i in range(7):
                ring_copy(p, way, i).wait_send()
            half_copy(p, way).wait_send()
            for h in range(2):
                full_copy(p, way, h).wait_send()
    for a in range(2):
        for k in (1, 2, 3):
            y_copy(a, k).wait_send()
        for i in range(4):
            x_copy(a, i).wait_send()
        for i in range(5):
            core_copy(a, i).wait_send()
    for k in range(1, NMP):
        p_copy(k).wait_send()


def gradients(lengths, x, g, wg, wu, wd, up_a, down_b, gain, up_b, down_a):
    vmem = pl.BlockSpec(memory_space=pltpu.VMEM)
    dma = pltpu.SemaphoreType.DMA
    return pl.pallas_call(
        gradients_kernel,
        out_shape=(
            jax.ShapeDtypeStruct((ADAPTER_RANK, ROWS), F32),
            jax.ShapeDtypeStruct((ADAPTER_RANK, SHARE), F32),
            jax.ShapeDtypeStruct((ADAPTER_RANK, SHARE), F32),
            jax.ShapeDtypeStruct((ADAPTER_RANK, ROWS), F32),
        ),
        in_specs=[pl.BlockSpec(memory_space=pltpu.SMEM), *[pl.BlockSpec(memory_space=pl.ANY)] * 7, *[vmem] * 3],
        out_specs=(vmem,) * 4,
        scratch_shapes=[
            pltpu.VMEM((SEQ, FEATS), BF),
            pltpu.VMEM((SEQ, FEATS), BF),
            pltpu.VMEM((3, ROWS, COLS), BF),
            pltpu.VMEM((2, ADAPTER_RANK, SEQ), BF),
            pltpu.VMEM((128, SEQ), F32),
            pltpu.VMEM((2, 128, WIDE), BF),
            dma((7,)),
            pltpu.VMEM((3, SEQ, WIDE), F32),
            pltpu.VMEM((NY, 2, ROWS, SEQ), BF),
            pltpu.VMEM((3, ROWS, WIDE), BF),
            pltpu.VMEM((FEATS, SEQ), F32),
            pltpu.VMEM((NY, 2, KLEN, SEQ), BF),
            pltpu.VMEM((3, KLEN, WIDE), BF),
            pltpu.VMEM((3, 2, 128, WIDE), BF),
            pltpu.VMEM((3, 2, SEQ, WIDE), BF),
            pltpu.VMEM((3, 2, 128, WIDE), F32),
            pltpu.VMEM((3, 2, 128, WIDE), BF),
            pltpu.VMEM((3, 2, SEQ, WIDE), BF),
            pltpu.VMEM((8, SEQ), F32),
            pltpu.VMEM((NMP, 8, SEQ), F32),
            pltpu.VMEM((2, 128, SEQ), F32),
            pltpu.VMEM((SEQ, WIDE), BF),
            pltpu.VMEM((2 * ADAPTER_RANK, WIDE), F32),
            pltpu.VMEM((2, ADAPTER_RANK, SEQ), BF),
            pltpu.VMEM((2, NMP, ADAPTER_RANK, SEQ), BF),
            pltpu.VMEM((8, 128), F32),
            pltpu.VMEM((NMP, 8, 128), F32),
            pltpu.VMEM((NDP, 16, 128), F32),
            pltpu.VMEM((NDP, 16, 128), BF),
            pltpu.VMEM((NDP, 16, 128), BF),
            pltpu.VMEM((8, 128), F32),
            pltpu.VMEM((NZ, 8, 128), F32),
            dma((4, 2, 7)),
            dma((4, 2, 7)),
            dma((2, 3)),
            dma((2, 3)),
            dma((2,)),
            dma((2, 4)),
            dma((2, 4)),
            dma((2, 5)),
            dma((2, 5)),
            dma((4, 2)),
            dma((4, 2)),
            dma((4, 2, 2)),
            dma((4, 2, 2)),
            dma((NMP - 1,)),
            dma((NMP - 1,)),
            dma((2, NMP - 1)),
            dma((2, NMP - 1)),
            dma((NMP - 1,)),
            dma((NMP - 1,)),
            dma((NDP,)),
            dma((NDP,)),
            dma((NMP,)),
            dma((NMP,)),
        ],
        compiler_params=pltpu.CompilerParams(collective_id=0, has_side_effects=True),
        name="gradients",
    )(lengths, x, g, wg, wu, wd, up_a, down_b, gain, up_b, down_a)


def per_device(
    residual_input,
    cotangent,
    lengths,
    norm_gain_vector,
    gate_projection_weight,
    up_projection_weight,
    down_projection_weight,
    up_adapter_first,
    up_adapter_second,
    down_adapter_first,
    down_adapter_second,
):
    up_a, up_b, down_a, down_b = gradients(
        lengths,
        residual_input,
        cotangent,
        gate_projection_weight,
        up_projection_weight,
        down_projection_weight,
        up_adapter_first.T,
        down_adapter_second,
        norm_gain_vector.reshape(MODEL_WIDTH // 128, 128),
        up_adapter_second,
        down_adapter_first.T,
    )
    return (up_a.T, up_b, down_a.T, down_b)


def solution(mesh):
    return jax.shard_map(
        per_device,
        mesh=mesh,
        in_specs=(
            P("dp", "mp"),
            P("dp", "mp"),
            P("dp"),
            P(),
            P("dp", "mp"),
            P("dp", "mp"),
            P("dp", "mp"),
            P(),
            P(None, "mp"),
            P("mp", None),
            P(),
        ),
        out_specs=(P("dp", None), P(None, ("mp", "dp")), P(("mp", "dp"), None), P(None, "dp")),
        check_vma=False,
    )
```

```python
import math

import jax
import jax.numpy as jnp
from jax import lax
from jax.experimental import pallas as pl
from jax.experimental.pallas import tpu as pltpu
from jax.sharding import PartitionSpec as P

MODEL_WIDTH = 5120
HIDDEN_SHARD = 6912
ADAPTER_RANK = 16

norm_eps = 1e-06
adapter_scale = 2.0
clip_coefficient = 0.005

NZ, NY, NX, NC = 8, 4, 4, 2
NMP = NX * NC
NDP = NZ * NY
ROWS = 160
KLEN = ROWS * NZ
SEQ = 256
COLS = 864
WIDE = 896
HALF = ROWS // 2

PIECES = ((0, 0, 0, 896), (1, 0, 0, 896), (2, 1, 384, 512), (2, 1, 0, 384))
RING = (((0, 0), (0, 1), (1, 0), (1, 1), (2, 0), (2, 1), (3, 0)), ((0, 0), (0, 1), (1, 0), (1, 1), (2, 0), (2, 1), (3, 1)))
ORDER = (
    *((0, i) for i in range(7)), *((1, i) for i in range(6)),
    (2, 0), (2, 1), (1, 6), (2, 2), (2, 3), (2, 4), (2, 5), (3, 0), (3, 1), (2, 6), (3, 2), (3, 3), (3, 4), (3, 5), (3, 6),
)
LANE0 = 768
SPOT = COLS - LANE0
FEATS = MODEL_WIDTH // NMP
FAR_FIRST = (4, 5, 3, 2, 6, 7, 1)
SHARE = COLS // NDP
MESH = pl.DeviceIdType.MESH
BF, F32 = jnp.bfloat16, jnp.float32


def contract_row_dims(left, right):
    return lax.dot_general(left, right, (((0,), (0,)), ((), ())), preferred_element_type=F32)


def contract_columns(left, right):
    return lax.dot_general(left, right, (((1,), (1,)), ((), ())), preferred_element_type=F32)


def remote(src, dst, send, recv, dp, mp):
    return pltpu.make_async_remote_copy(
        src_ref=src, dst_ref=dst, send_sem=send, recv_sem=recv, device_id={"dp": dp, "mp": mp}, device_id_type=MESH
    )


def signal(sem, dp, mp):
    pl.semaphore_signal(sem, inc=1, device_id={"dp": dp, "mp": mp}, device_id_type=MESH)


def gradients_kernel(
    lengths, x_in, g_in, w0_in, w1_in, w2_in, up_a, down_b, gain, up_b, down_a, u_out, s_out,
    xin, gin, win, window, turn, ad, lsem, c, at, wb, xt, a_all, b_all, cs2, cs1, near, cr2, cr1, ps, p_all, lat, hid, full, v, v_all, q, q_all, part, msg, msg_all, us, u_row,
    bs, br, ays, ayr, loc, axs, axr, ads, adr, c2s, c2r, c1s, c1r, pss, psr, vs, vr, qs, qr, ms, mr, us4, ur4,
):
    d, m = lax.axis_index("dp"), lax.axis_index("mp")
    z, y, x, core = d // NY, lax.rem(d, NY), m // NC, lax.rem(m, NC)

    def dp_of(zz, yy):
        return lax.rem(zz, NZ) * NY + lax.rem(yy, NY)

    def mp_of(xx, cc):
        return lax.rem(xx, NX) * NC + cc

    up_z, down_z = dp_of(z + 1, y), dp_of(z + NZ - 1, y)
    up_y, down_y = dp_of(z, y + 1), dp_of(z, y + NY - 1)
    up_x, down_x = mp_of(x + 1, core), mp_of(x + NX - 1, core)
    far_x = mp_of(x + 2, core)
    twin = mp_of(x, 1 - core)

    bar = pltpu.get_barrier_semaphore()
    signal(bar, up_z, m)
    signal(bar, down_z, m)
    for k in range(1, NY):
        signal(bar, dp_of(z, y + k), m)
    for k in range(1, NMP):
        signal(bar, d, lax.rem(m + k, NMP))

    lanes = pl.ds(pl.multiple_of(d * (ROWS // 32) // 4 * 128, 128), SEQ)
    loads = (
        (w0_in, win.at[0]),
        (x_in, xin),
        (w1_in, win.at[1]),
        (g_in, gin),
        (w2_in, win.at[2]),
        (up_a.at[:, lanes], window.at[0]),
        (down_b.at[:, lanes], window.at[1]),
    )

    def load(i):
        return pltpu.make_async_copy(*loads[i], lsem.at[i])

    for i in range(len(loads)):
        load(i).start()

    def adapter_rows(i):
        wide = window[i].astype(F32)
        rows = jnp.zeros((ADAPTER_RANK, ROWS), F32)
        for k in range(NY):
            rows = rows + jnp.where(y == k, wide[:, 32 * k : 32 * k + ROWS], 0.0)
        turn[...] = jnp.zeros_like(turn)
        turn[SPOT : SPOT + ADAPTER_RANK, :ROWS] = rows
        return turn[...].T[:ROWS].astype(BF)

    def assemble(w, beside):
        wb[w, :, :COLS] = win[w]
        tile = wb[w, :, LANE0:]
        lane = lax.broadcasted_iota(jnp.int32, tile.shape, 1)
        wb[w, :, LANE0:] = jnp.where(lane < SPOT, tile, beside)

    load(0).wait()
    assemble(0, jnp.zeros((ROWS, 128), BF))
    pl.semaphore_wait(bar, 2 + NY - 1 + NMP - 1)

    def rows_of(zz, h, n):
        return pl.ds(pl.multiple_of(zz * ROWS + h * HALF, 16), n)

    def ring_copy(p, way, i):
        w, _, c0, n = PIECES[p]
        s, h = RING[way][i]
        src_z = lax.rem(z + (NZ - s if way == 0 else s), NZ)
        cols = pl.ds(c0, n)
        here = wb.at[w, pl.ds(h * HALF, HALF), cols] if s == 0 else b_all.at[w, rows_of(src_z, h, HALF), cols]
        there = b_all.at[w, rows_of(src_z, h, HALF), cols]
        return remote(here, there, bs.at[p, way, i], br.at[p, way, i], up_z if way == 0 else down_z, m)

    def ring_issue(p, i):
        for way in range(2):
            s, h = RING[way][i]
            if s:
                ring_copy(p, way, 2 * (s - 1) + h).wait_recv()
            ring_copy(p, way, i).start()

    def ring_finish(p):
        for way in range(2):
            for i in (5, 6) if way == 0 else (4, 6):
                ring_copy(p, way, i).wait_recv()

    def feats(mm):
        return pl.ds(pl.multiple_of(mm * ROWS, 16), ROWS)

    def y_copy(a, k):
        yy = lax.rem(y + k, NY)
        return remote(at.at[yy, a], a_all.at[y, a, feats(m), :], ays.at[a, k - 1], ayr.at[a, k - 1], dp_of(z, yy), m)

    def own_copy(a):
        return pltpu.make_async_copy(at.at[y, a], a_all.at[y, a, feats(m), :], loc.at[a])

    def block(a, mm, e0, ne):
        return a_all.at[pl.ds(e0, ne), a, feats(mm), :]

    def x_copy(a, i):
        mm, e0, ne, to = ((m, 0, 4, up_x), (m, 0, 4, down_x), (down_x, 0, 2, up_x), (up_x, 2, 2, down_x))[i]
        return remote(block(a, mm, e0, ne), block(a, mm, e0, ne), axs.at[a, i], axr.at[a, i], d, to)

    def core_copy(a, i):
        mm, e0, ne = ((m, 0, 4), (down_x, 0, 4), (up_x, 0, 4), (far_x, 0, 2), (far_x, 2, 2))[i]
        return remote(block(a, mm, e0, ne), block(a, mm, e0, ne), ads.at[a, i], adr.at[a, i], d, twin)

    def tokens_start(a):
        for k in (2, 1, 3):
            y_copy(a, k).start()
        own_copy(a).start()

    def tokens_x(a):
        own_copy(a).wait()
        for k in (1, 2, 3):
            y_copy(a, k).wait_recv()
        x_copy(a, 0).start()
        x_copy(a, 1).start()
        core_copy(a, 0).start()

    def tokens_on(a):
        x_copy(a, 0).wait_recv()
        x_copy(a, 2).start()
        x_copy(a, 1).wait_recv()
        x_copy(a, 3).start()
        core_copy(a, 1).start()
        core_copy(a, 2).start()

    def tokens_last(a):
        x_copy(a, 2).wait_recv()
        core_copy(a, 3).start()
        x_copy(a, 3).wait_recv()
        core_copy(a, 4).start()

    def tokens_done(a):
        for i in range(5):
            core_copy(a, i).wait_recv()

    def product(p, t, store):
        w, a, c0, n = PIECES[p]

        def tile(lo, size):
            acc = lax.dot_general(
                a_all[t, a], b_all[w, :, pl.ds(lo, size)], (((0,), (0,)), ((), ())), preferred_element_type=F32
            )
            store(w, lo, size, acc)

        def step(i, carry):
            tile(pl.multiple_of(c0 + i * 256, 128), 256)
            return carry

        lax.fori_loop(0, n // 256, step, 0)
        if n % 256:
            tile(c0 + n - n % 256, n % 256)

    def half_copy(p, way):
        w, _, c0, n = PIECES[p]
        cols = pl.ds(c0, n)
        return remote(
            cs2.at[w, way, :, cols], cr2.at[w, way, :, cols], c2s.at[p, way], c2r.at[p, way], up_y if way == 0 else down_y, m
        )

    def full_copy(p, way, h):
        w, _, c0, n = PIECES[p]
        part = (way, pl.ds(h * 128, 128), pl.ds(c0, n))
        return remote(
            cs1.at[(w, *part)], cr1.at[(w, *part)], c1s.at[p, way, h], c1r.at[p, way, h], up_y if way == 0 else down_y, m
        )

    def unit_far(p):
        def store(w, lo, size, acc):
            v = acc.astype(BF)
            cs2[w, 0, :, pl.ds(lo, size)] = v[:128]
            cs2[w, 1, :, pl.ds(lo, size)] = v[128:]

        product(p, lax.rem(y + 2, NY), store)
        half_copy(p, 0).start()
        half_copy(p, 1).start()

    def unit_near(p, way):
        def store(w, lo, size, acc):
            sent, kept = (acc[128:], acc[:128]) if way == 0 else (acc[:128], acc[128:])
            cs1[w, way, pl.ds((1 - way) * 128, 128), pl.ds(lo, size)] = sent.astype(BF)
            near[w, way, :, pl.ds(lo, size)] = kept

        product(p, lax.rem(y + (1 if way == 0 else NY - 1), NY), store)
        full_copy(p, way, 1 - way).start()

    def unit_pass(p):
        w, _, c0, n = PIECES[p]
        for way in range(2):
            half_copy(p, way).wait_recv()
            at_rows, cols = pl.ds(way * 128, 128), pl.ds(c0, n)
            total = near[w, way, :, cols] + cr2[w, way, :, cols].astype(F32)
            cs1[w, way, at_rows, cols] = total.astype(BF)
            full_copy(p, way, way).start()

    def unit_own(p):
        def store(w, lo, size, acc):
            c[w, :, pl.ds(lo, size)] = acc

        product(p, y, store)

    def unit_sum(p):
        w, _, c0, n = PIECES[p]
        cols = pl.ds(c0, n)
        for way in range(2):
            for h in range(2):
                full_copy(p, way, h).wait_recv()
        c[w, :, cols] += cr1[w, 0, :, cols].astype(F32) + cr1[w, 1, :, cols].astype(F32)

    def p_copy(k):
        return remote(ps, p_all.at[m], pss.at[k - 1], psr.at[k - 1], d, lax.rem(m + k, NMP))

    def own_rows():
        for w in range(3):
            b_all[w, rows_of(z, 0, ROWS), :] = wb[w]

    def normalize():
        p_all[m] = ps[...]
        for k in range(1, NMP):
            p_copy(k).wait_recv()
        inverse = lax.rsqrt(jnp.sum(p_all[...], axis=0)[:1] * (1.0 / MODEL_WIDTH) + norm_eps)
        gains = gain[...].astype(F32).T
        lane = lax.broadcasted_iota(jnp.int32, gains.shape, 1)
        column = jnp.concatenate(
            [
                jnp.sum(jnp.where(lane == m * (FEATS // 128) + i, gains, 0.0), axis=1, keepdims=True)
                for i in range(FEATS // 128)
            ],
            axis=0,
        )
        normed = (xt[...] * inverse * column).astype(BF)
        for yy in range(NY):
            at[yy, 0] = normed[yy * ROWS : (yy + 1) * ROWS]

    def mask():
        token = lax.broadcasted_iota(jnp.int32, (1, SEQ), 1)
        live = (token < lengths[0]).astype(F32)
        masked = (gin[...].astype(F32).T * live).astype(BF)
        for yy in range(NY):
            at[yy, 1] = masked[yy * ROWS : (yy + 1) * ROWS]

    def tokens_first():
        load(1).wait()
        xt[...] = xin[...].astype(F32).T
        ps[...] = jnp.broadcast_to(jnp.sum(xt[...] * xt[...], axis=0, keepdims=True), ps.shape)
        for k in FAR_FIRST:
            p_copy(k).start()
        load(2).wait()
        load(5).wait()
        assemble(1, adapter_rows(0))
        normalize()
        tokens_start(0)

    def tokens_second():
        load(3).wait()
        mask()
        tokens_start(1)

    def weights_rest():
        load(4).wait()
        load(6).wait()
        assemble(2, adapter_rows(1))
        own_rows()

    def adapters_rest():
        part[...] = jnp.zeros_like(part)
        ad[...] = jnp.zeros_like(ad)
        ad[0, SPOT : SPOT + ADAPTER_RANK, :COLS] = up_b[...]
        ad[1, SPOT : SPOT + ADAPTER_RANK, :COLS] = down_a[...]

    def tile_of(i):
        return pl.ds(pl.multiple_of(i * 128, 128), 128)

    def spots(a):
        return a[SPOT : SPOT + ADAPTER_RANK]

    def forward_side():
        up_latent = c[1, :, LANE0:].astype(BF)
        lat[...] = jnp.zeros_like(lat)

        def chunk(i, carry):
            cols = tile_of(i)
            gate_act = jax.nn.silu(c[0, :, cols])
            c[0, :, cols] = gate_act
            up = c[1, :, cols] + adapter_scale * jnp.dot(up_latent, ad[0, :, cols], preferred_element_type=F32)
            hidden = (gate_act * up).astype(BF)
            hid[:, cols] = hidden
            lat[0] += contract_columns(ad[1, :, cols], hidden)
            return carry

        lax.fori_loop(0, WIDE // 128, chunk, 0)
        v[0] = spots(lat[0]).astype(BF)
        for k in FAR_FIRST:
            v_copy(0, k).start()

    def down_side():
        v_all[0, m] = v[0]
        for k in range(1, NMP):
            v_copy(0, k).wait_recv()
        latent = jnp.sum(v_all[0].astype(F32), axis=0).astype(BF)
        for yy in range(NY):
            put(yy, 4, adapter_scale * contract_columns(latent, at[yy, 1]))

    def backward_side(lo, hi):
        up_latent = c[1, :, LANE0:].astype(BF)
        back_latent = c[2, :, LANE0:].astype(BF)

        def chunk(i, carry):
            cols = tile_of(i)
            back = c[2, :, cols] + adapter_scale * jnp.dot(back_latent, ad[1, :, cols], preferred_element_type=F32)
            up_gradient = (back * c[0, :, cols]).astype(BF)
            lat[1] += contract_columns(ad[0, :, cols], up_gradient)
            full[:ADAPTER_RANK, cols] = adapter_scale * spots(contract_row_dims(back_latent, hid[:, cols]))
            full[ADAPTER_RANK:, cols] = adapter_scale * spots(contract_row_dims(up_latent, up_gradient))
            return carry

        lax.fori_loop(lo, hi, chunk, 0)

    def v_copy(i, k):
        return remote(v.at[i], v_all.at[i, m], vs.at[i, k - 1], vr.at[i, k - 1], d, lax.rem(m + k, NMP))

    def q_copy(k):
        return remote(q, q_all.at[m], qs.at[k - 1], qr.at[k - 1], d, lax.rem(m + k, NMP))

    def put(yy, j0, rows):
        for j in range(4):
            part[(j0 + j) * NY + yy, 8:12] = rows[4 * j : 4 * j + 4, :128]
            part[(j0 + j) * NY + yy, 12:16, : ROWS - 128] = rows[4 * j : 4 * j + 4, 128:]

    plan = {
        1: [tokens_first],
        2: [tokens_second],
        3: [lambda: tokens_x(0)],
        4: [weights_rest],
        5: [adapters_rest],
        6: [lambda: tokens_on(0), lambda: tokens_x(1)],
        8: [lambda: tokens_last(0)],
        9: [lambda: ring_finish(0), lambda: tokens_done(0), lambda: unit_far(0)],
        10: [lambda: unit_near(0, 0)],
        11: [lambda: unit_near(0, 1)],
        12: [lambda: tokens_on(1), lambda: unit_pass(0)],
        13: [lambda: unit_own(0)],
        14: [lambda: tokens_last(1)],
        18: [lambda: ring_finish(1), lambda: unit_far(1)],
        19: [lambda: unit_near(1, 0)],
        20: [lambda: unit_near(1, 1)],
        21: [lambda: unit_sum(0)],
        22: [lambda: unit_pass(1)],
        23: [lambda: unit_own(1), lambda: tokens_done(1)],
        25: [lambda: ring_finish(2), lambda: unit_far(2)],
        26: [lambda: unit_near(2, 0)],
        27: [lambda: unit_near(2, 1)],
    }
    for at_position, (p, i) in enumerate(ORDER):
        ring_issue(p, i)
        for u in plan.get(at_position, ()):
            u()
    ring_finish(3)
    unit_far(3)
    unit_near(3, 0)
    unit_near(3, 1)
    unit_pass(2)
    unit_own(2)
    unit_own(3)
    unit_pass(3)
    unit_sum(1)
    forward_side()
    unit_sum(2)
    backward_side(3, WIDE // 128)
    unit_sum(3)
    backward_side(0, 3)
    v[1] = spots(lat[1]).astype(BF)
    for k in FAR_FIRST:
        v_copy(1, k).start()
    v_all[1, m] = v[1]
    down_side()

    for i in range(NDP):
        for r in range(4):
            part[i, :8, r * 32 : r * 32 + 32] = full[r * 8 : r * 8 + 8, i * SHARE : i * SHARE + 32]
    squares = jnp.sum(full[...] * full[...], keepdims=True)
    for k in range(1, NMP):
        v_copy(1, k).wait_recv()
    latent = jnp.sum(v_all[1].astype(F32), axis=0).astype(BF)
    for yy in range(NY):
        put(yy, 0, adapter_scale * contract_columns(latent, at[yy, 0]))
    features = part[:, 8:, :]
    squares = squares + jnp.sum(jnp.sum(features * features, axis=0), keepdims=True)
    q[...] = jnp.broadcast_to(squares, q.shape)
    for k in FAR_FIRST:
        q_copy(k).start()
    q_all[m] = q[...]
    for k in range(1, NMP):
        q_copy(k).wait_recv()
    clip_limit = clip_coefficient * math.sqrt(2.0 * ADAPTER_RANK * (MODEL_WIDTH + HIDDEN_SHARD))
    norm = jnp.sqrt(jnp.sum(q_all[...], axis=0))
    factor = jnp.minimum(1.0, clip_limit / (norm + 1e-06))[:1, :1]
    msg[...] = (part[...] * factor[None]).astype(BF)

    def m_copy(k):
        dd = lax.rem(d + k, NDP)
        return remote(msg.at[dd], msg_all.at[d], ms.at[k], mr.at[d], dd, m)

    def m_arrive(k, carry):
        dd = lax.rem(d + k, NDP)
        remote(msg.at[0], msg_all.at[dd], ms.at[k], mr.at[dd], dd, m).wait_recv()
        return carry

    for i in range(NDP - 1):
        m_copy((i + 12) % (NDP - 1) + 1).start()
    msg_all[d] = msg[d]
    lax.fori_loop(1, NDP, m_arrive, 0)
    summed = jnp.sum(msg_all[...].astype(F32), axis=0)
    us[...] = summed[8:]

    goal = m * NY + y
    here = z == m

    def u_copy(k):
        return remote(us, u_row.at[z], us4.at[k], ur4.at[z], goal, lax.rem(m + k, NMP))

    for k in range(1, NMP):
        u_copy(k).start()

    @pl.when(jnp.logical_not(here))
    def _():
        u_copy(0).start()

    @pl.when(here)
    def _():
        u_row[z] = us[...]

    for r in range(4):
        s_out[r * 8 : r * 8 + 8] = summed[:8, r * 32 : r * 32 + SHARE]

    for j in range(NZ):
        @pl.when(jnp.logical_not(jnp.logical_and(here, z == j)))
        def _():
            remote(us, u_row.at[j], us4.at[0], ur4.at[j], goal, lax.rem(m + 1, NMP)).wait_recv()

        u_out[4 * j : 4 * j + 4, :128] = u_row[j, :4]
        u_out[4 * j : 4 * j + 4, 128:] = u_row[j, 4:, : ROWS - 128]

    def m_sent(k, carry):
        m_copy(k).wait_send()
        return carry

    lax.fori_loop(1, NDP, m_sent, 0)
    for k in range(1, NMP):
        v_copy(0, k).wait_send()
        v_copy(1, k).wait_send()
        q_copy(k).wait_send()
        u_copy(k).wait_send()

    @pl.when(jnp.logical_not(here))
    def _():
        u_copy(0).wait_send()

    for p in range(4):
        for way in range(2):
            for i in range(7):
                ring_copy(p, way, i).wait_send()
            half_copy(p, way).wait_send()
            for h in range(2):
                full_copy(p, way, h).wait_send()
    for a in range(2):
        for k in (1, 2, 3):
            y_copy(a, k).wait_send()
        for i in range(4):
            x_copy(a, i).wait_send()
        for i in range(5):
            core_copy(a, i).wait_send()
    for k in range(1, NMP):
        p_copy(k).wait_send()


def gradients(lengths, x, g, wg, wu, wd, up_a, down_b, gain, up_b, down_a):
    vmem = pl.BlockSpec(memory_space=pltpu.VMEM)
    dma = pltpu.SemaphoreType.DMA
    return pl.pallas_call(
        gradients_kernel,
        out_shape=(
            jax.ShapeDtypeStruct((2 * ADAPTER_RANK, ROWS), F32),
            jax.ShapeDtypeStruct((2 * ADAPTER_RANK, SHARE), F32),
        ),
        in_specs=[pl.BlockSpec(memory_space=pltpu.SMEM), *[pl.BlockSpec(memory_space=pl.ANY)] * 7, *[vmem] * 3],
        out_specs=(vmem, vmem),
        scratch_shapes=[
            pltpu.VMEM((SEQ, FEATS), BF),
            pltpu.VMEM((SEQ, FEATS), BF),
            pltpu.VMEM((3, ROWS, COLS), BF),
            pltpu.VMEM((2, ADAPTER_RANK, SEQ), BF),
            pltpu.VMEM((128, SEQ), F32),
            pltpu.VMEM((2, 128, WIDE), BF),
            dma((7,)),
            pltpu.VMEM((3, SEQ, WIDE), F32),
            pltpu.VMEM((NY, 2, ROWS, SEQ), BF),
            pltpu.VMEM((3, ROWS, WIDE), BF),
            pltpu.VMEM((FEATS, SEQ), F32),
            pltpu.VMEM((NY, 2, KLEN, SEQ), BF),
            pltpu.VMEM((3, KLEN, WIDE), BF),
            pltpu.VMEM((3, 2, 128, WIDE), BF),
            pltpu.VMEM((3, 2, SEQ, WIDE), BF),
            pltpu.VMEM((3, 2, 128, WIDE), F32),
            pltpu.VMEM((3, 2, 128, WIDE), BF),
            pltpu.VMEM((3, 2, SEQ, WIDE), BF),
            pltpu.VMEM((8, SEQ), F32),
            pltpu.VMEM((NMP, 8, SEQ), F32),
            pltpu.VMEM((2, 128, SEQ), F32),
            pltpu.VMEM((SEQ, WIDE), BF),
            pltpu.VMEM((2 * ADAPTER_RANK, WIDE), F32),
            pltpu.VMEM((2, ADAPTER_RANK, SEQ), BF),
            pltpu.VMEM((2, NMP, ADAPTER_RANK, SEQ), BF),
            pltpu.VMEM((8, 128), F32),
            pltpu.VMEM((NMP, 8, 128), F32),
            pltpu.VMEM((NDP, 16, 128), F32),
            pltpu.VMEM((NDP, 16, 128), BF),
            pltpu.VMEM((NDP, 16, 128), BF),
            pltpu.VMEM((8, 128), F32),
            pltpu.VMEM((NZ, 8, 128), F32),
            dma((4, 2, 7)),
            dma((4, 2, 7)),
            dma((2, 3)),
            dma((2, 3)),
            dma((2,)),
            dma((2, 4)),
            dma((2, 4)),
            dma((2, 5)),
            dma((2, 5)),
            dma((4, 2)),
            dma((4, 2)),
            dma((4, 2, 2)),
            dma((4, 2, 2)),
            dma((NMP - 1,)),
            dma((NMP - 1,)),
            dma((2, NMP - 1)),
            dma((2, NMP - 1)),
            dma((NMP - 1,)),
            dma((NMP - 1,)),
            dma((NDP,)),
            dma((NDP,)),
            dma((NMP,)),
            dma((NMP,)),
        ],
        compiler_params=pltpu.CompilerParams(collective_id=0, has_side_effects=True),
        name="gradients",
    )(lengths, x, g, wg, wu, wd, up_a, down_b, gain, up_b, down_a)


def hand_over_kernel(u, s, up_a, up_b, down_a, down_b):
    up_a[...] = u[:ADAPTER_RANK]
    down_b[...] = u[ADAPTER_RANK:]
    down_a[...] = s[:ADAPTER_RANK]
    up_b[...] = s[ADAPTER_RANK:]


def hand_over(u, s):
    vmem = pl.BlockSpec(memory_space=pltpu.VMEM)
    of_u = jax.ShapeDtypeStruct((ADAPTER_RANK, ROWS), F32)
    of_s = jax.ShapeDtypeStruct((ADAPTER_RANK, SHARE), F32)
    return pl.pallas_call(
        hand_over_kernel, out_shape=(of_u, of_s, of_s, of_u), in_specs=[vmem] * 2, out_specs=(vmem,) * 4, name="hand_over"
    )(u, s)


def per_device(
    residual_input,
    cotangent,
    lengths,
    norm_gain_vector,
    gate_projection_weight,
    up_projection_weight,
    down_projection_weight,
    up_adapter_first,
    up_adapter_second,
    down_adapter_first,
    down_adapter_second,
):
    u, s = gradients(
        lengths,
        residual_input,
        cotangent,
        gate_projection_weight,
        up_projection_weight,
        down_projection_weight,
        up_adapter_first.T,
        down_adapter_second,
        norm_gain_vector.reshape(MODEL_WIDTH // 128, 128),
        up_adapter_second,
        down_adapter_first.T,
    )
    up_a, up_b, down_a, down_b = hand_over(u, s)
    return (up_a.T, up_b, down_a.T, down_b)


def solution(mesh):
    return jax.shard_map(
        per_device,
        mesh=mesh,
        in_specs=(
            P("dp", "mp"),
            P("dp", "mp"),
            P("dp"),
            P(),
            P("dp", "mp"),
            P("dp", "mp"),
            P("dp", "mp"),
            P(),
            P(None, "mp"),
            P("mp", None),
            P(),
        ),
        out_specs=(P("dp", None), P(None, ("mp", "dp")), P(("mp", "dp"), None), P(None, "dp")),
        check_vma=False,
    )
```

```python
import math

import jax
import jax.numpy as jnp
from jax import lax
from jax.experimental import pallas as pl
from jax.experimental.pallas import tpu as pltpu
from jax.sharding import PartitionSpec as P

MODEL_WIDTH = 5120
HIDDEN_SHARD = 6912
ADAPTER_RANK = 16

norm_eps = 1e-06
adapter_scale = 2.0
clip_coefficient = 0.005

NZ, NY, NX, NC = 8, 4, 4, 2
NMP = NX * NC
NDP = NZ * NY
ROWS = 160
KLEN = ROWS * NZ
SEQ = 256
COLS = 864
WIDE = 896
HALF = ROWS // 2

PIECES = ((0, 0, 0, 896), (1, 0, 0, 896), (2, 1, 384, 512), (2, 1, 0, 384))
RING = (((0, 0), (0, 1), (1, 0), (1, 1), (2, 0), (2, 1), (3, 0)), ((0, 0), (0, 1), (1, 0), (1, 1), (2, 0), (2, 1), (3, 1)))
ORDER = (
    *((0, i) for i in range(7)), *((1, i) for i in range(6)),
    (2, 0), (2, 1), (1, 6), (2, 2), (2, 3), (2, 4), (2, 5), (3, 0), (3, 1), (2, 6), (3, 2), (3, 3), (3, 4), (3, 5), (3, 6),
)
LANE0 = 768
SPOT = COLS - LANE0
FEATS = MODEL_WIDTH // NMP
FAR_FIRST = (4, 5, 3, 2, 6, 7, 1)
SHARE = COLS // NDP
MESH = pl.DeviceIdType.MESH
BF, F32 = jnp.bfloat16, jnp.float32


def contract_row_dims(left, right):
    return lax.dot_general(left, right, (((0,), (0,)), ((), ())), preferred_element_type=F32)


def contract_columns(left, right):
    return lax.dot_general(left, right, (((1,), (1,)), ((), ())), preferred_element_type=F32)


def remote(src, dst, send, recv, dp, mp):
    return pltpu.make_async_remote_copy(
        src_ref=src, dst_ref=dst, send_sem=send, recv_sem=recv, device_id={"dp": dp, "mp": mp}, device_id_type=MESH
    )


def signal(sem, dp, mp):
    pl.semaphore_signal(sem, inc=1, device_id={"dp": dp, "mp": mp}, device_id_type=MESH)


def gradients_kernel(
    lengths, x_in, g_in, w0_in, w1_in, w2_in, up_a, down_b, gain, up_b, down_a, u_out, s_out,
    xin, gin, win, window, turn, ad, lsem, c, at, wb, xt, a_all, b_all, cs2, cs1, near, cr2, cr1, ps, p_all, lat, hid, full, v, v_all, q, q_all, part, msg, msg_all, factor, factor_all, us, u_row,
    bs, br, ays, ayr, loc, axs, axr, ads, adr, c2s, c2r, c1s, c1r, pss, psr, vs, vr, qs, qr, ms, mr, fs, fr, us4, ur4,
):
    d, m = lax.axis_index("dp"), lax.axis_index("mp")
    z, y, x, core = d // NY, lax.rem(d, NY), m // NC, lax.rem(m, NC)

    def dp_of(zz, yy):
        return lax.rem(zz, NZ) * NY + lax.rem(yy, NY)

    def mp_of(xx, cc):
        return lax.rem(xx, NX) * NC + cc

    up_z, down_z = dp_of(z + 1, y), dp_of(z + NZ - 1, y)
    up_y, down_y = dp_of(z, y + 1), dp_of(z, y + NY - 1)
    up_x, down_x = mp_of(x + 1, core), mp_of(x + NX - 1, core)
    far_x = mp_of(x + 2, core)
    twin = mp_of(x, 1 - core)

    bar = pltpu.get_barrier_semaphore()
    signal(bar, up_z, m)
    signal(bar, down_z, m)
    for k in range(1, NY):
        signal(bar, dp_of(z, y + k), m)
    for k in range(1, NMP):
        signal(bar, d, lax.rem(m + k, NMP))

    lanes = pl.ds(pl.multiple_of(d * (ROWS // 32) // 4 * 128, 128), SEQ)
    loads = (
        (w0_in, win.at[0]),
        (x_in, xin),
        (w1_in, win.at[1]),
        (g_in, gin),
        (w2_in, win.at[2]),
        (up_a.at[:, lanes], window.at[0]),
        (down_b.at[:, lanes], window.at[1]),
    )

    def load(i):
        return pltpu.make_async_copy(*loads[i], lsem.at[i])

    for i in range(len(loads)):
        load(i).start()

    def adapter_rows(i):
        wide = window[i].astype(F32)
        rows = jnp.zeros((ADAPTER_RANK, ROWS), F32)
        for k in range(NY):
            rows = rows + jnp.where(y == k, wide[:, 32 * k : 32 * k + ROWS], 0.0)
        turn[...] = jnp.zeros_like(turn)
        turn[SPOT : SPOT + ADAPTER_RANK, :ROWS] = rows
        return turn[...].T[:ROWS].astype(BF)

    def assemble(w, beside):
        wb[w, :, :COLS] = win[w]
        tile = wb[w, :, LANE0:]
        lane = lax.broadcasted_iota(jnp.int32, tile.shape, 1)
        wb[w, :, LANE0:] = jnp.where(lane < SPOT, tile, beside)

    load(0).wait()
    assemble(0, jnp.zeros((ROWS, 128), BF))
    pl.semaphore_wait(bar, 2 + NY - 1 + NMP - 1)

    def rows_of(zz, h, n):
        return pl.ds(pl.multiple_of(zz * ROWS + h * HALF, 16), n)

    def ring_copy(p, way, i):
        w, _, c0, n = PIECES[p]
        s, h = RING[way][i]
        src_z = lax.rem(z + (NZ - s if way == 0 else s), NZ)
        cols = pl.ds(c0, n)
        here = wb.at[w, pl.ds(h * HALF, HALF), cols] if s == 0 else b_all.at[w, rows_of(src_z, h, HALF), cols]
        there = b_all.at[w, rows_of(src_z, h, HALF), cols]
        return remote(here, there, bs.at[p, way, i], br.at[p, way, i], up_z if way == 0 else down_z, m)

    def ring_issue(p, i):
        for way in range(2):
            s, h = RING[way][i]
            if s:
                ring_copy(p, way, 2 * (s - 1) + h).wait_recv()
            ring_copy(p, way, i).start()

    def ring_finish(p):
        for way in range(2):
            for i in (5, 6) if way == 0 else (4, 6):
                ring_copy(p, way, i).wait_recv()

    def feats(mm):
        return pl.ds(pl.multiple_of(mm * ROWS, 16), ROWS)

    def y_copy(a, k):
        yy = lax.rem(y + k, NY)
        return remote(at.at[yy, a], a_all.at[y, a, feats(m), :], ays.at[a, k - 1], ayr.at[a, k - 1], dp_of(z, yy), m)

    def own_copy(a):
        return pltpu.make_async_copy(at.at[y, a], a_all.at[y, a, feats(m), :], loc.at[a])

    def block(a, mm, e0, ne):
        return a_all.at[pl.ds(e0, ne), a, feats(mm), :]

    def x_copy(a, i):
        mm, e0, ne, to = ((m, 0, 4, up_x), (m, 0, 4, down_x), (down_x, 0, 2, up_x), (up_x, 2, 2, down_x))[i]
        return remote(block(a, mm, e0, ne), block(a, mm, e0, ne), axs.at[a, i], axr.at[a, i], d, to)

    def core_copy(a, i):
        mm, e0, ne = ((m, 0, 4), (down_x, 0, 4), (up_x, 0, 4), (far_x, 0, 2), (far_x, 2, 2))[i]
        return remote(block(a, mm, e0, ne), block(a, mm, e0, ne), ads.at[a, i], adr.at[a, i], d, twin)

    def tokens_start(a):
        for k in (2, 1, 3):
            y_copy(a, k).start()
        own_copy(a).start()

    def tokens_x(a):
        own_copy(a).wait()
        for k in (1, 2, 3):
            y_copy(a, k).wait_recv()
        x_copy(a, 0).start()
        x_copy(a, 1).start()
        core_copy(a, 0).start()

    def tokens_on(a):
        x_copy(a, 0).wait_recv()
        x_copy(a, 2).start()
        x_copy(a, 1).wait_recv()
        x_copy(a, 3).start()
        core_copy(a, 1).start()
        core_copy(a, 2).start()

    def tokens_last(a):
        x_copy(a, 2).wait_recv()
        core_copy(a, 3).start()
        x_copy(a, 3).wait_recv()
        core_copy(a, 4).start()

    def tokens_done(a):
        for i in range(5):
            core_copy(a, i).wait_recv()

    def product(p, t, store):
        w, a, c0, n = PIECES[p]

        def tile(lo, size):
            acc = lax.dot_general(
                a_all[t, a], b_all[w, :, pl.ds(lo, size)], (((0,), (0,)), ((), ())), preferred_element_type=F32
            )
            store(w, lo, size, acc)

        def step(i, carry):
            tile(pl.multiple_of(c0 + i * 256, 128), 256)
            return carry

        lax.fori_loop(0, n // 256, step, 0)
        if n % 256:
            tile(c0 + n - n % 256, n % 256)

    def half_copy(p, way):
        w, _, c0, n = PIECES[p]
        cols = pl.ds(c0, n)
        return remote(
            cs2.at[w, way, :, cols], cr2.at[w, way, :, cols], c2s.at[p, way], c2r.at[p, way], up_y if way == 0 else down_y, m
        )

    def full_copy(p, way, h):
        w, _, c0, n = PIECES[p]
        part = (way, pl.ds(h * 128, 128), pl.ds(c0, n))
        return remote(
            cs1.at[(w, *part)], cr1.at[(w, *part)], c1s.at[p, way, h], c1r.at[p, way, h], up_y if way == 0 else down_y, m
        )

    def unit_far(p):
        def store(w, lo, size, acc):
            v = acc.astype(BF)
            cs2[w, 0, :, pl.ds(lo, size)] = v[:128]
            cs2[w, 1, :, pl.ds(lo, size)] = v[128:]

        product(p, lax.rem(y + 2, NY), store)
        half_copy(p, 0).start()
        half_copy(p, 1).start()

    def unit_near(p, way):
        def store(w, lo, size, acc):
            sent, kept = (acc[128:], acc[:128]) if way == 0 else (acc[:128], acc[128:])
            cs1[w, way, pl.ds((1 - way) * 128, 128), pl.ds(lo, size)] = sent.astype(BF)
            near[w, way, :, pl.ds(lo, size)] = kept

        product(p, lax.rem(y + (1 if way == 0 else NY - 1), NY), store)
        full_copy(p, way, 1 - way).start()

    def unit_pass(p):
        w, _, c0, n = PIECES[p]
        for way in range(2):
            half_copy(p, way).wait_recv()
            at_rows, cols = pl.ds(way * 128, 128), pl.ds(c0, n)
            total = near[w, way, :, cols] + cr2[w, way, :, cols].astype(F32)
            cs1[w, way, at_rows, cols] = total.astype(BF)
            full_copy(p, way, way).start()

    def unit_own(p):
        def store(w, lo, size, acc):
            c[w, :, pl.ds(lo, size)] = acc

        product(p, y, store)

    def unit_sum(p):
        w, _, c0, n = PIECES[p]
        cols = pl.ds(c0, n)
        for way in range(2):
            for h in range(2):
                full_copy(p, way, h).wait_recv()
        c[w, :, cols] += cr1[w, 0, :, cols].astype(F32) + cr1[w, 1, :, cols].astype(F32)

    def p_copy(k):
        return remote(ps, p_all.at[m], pss.at[k - 1], psr.at[k - 1], d, lax.rem(m + k, NMP))

    def own_rows():
        for w in range(3):
            b_all[w, rows_of(z, 0, ROWS), :] = wb[w]

    def normalize():
        p_all[m] = ps[...]
        for k in range(1, NMP):
            p_copy(k).wait_recv()
        inverse = lax.rsqrt(jnp.sum(p_all[...], axis=0)[:1] * (1.0 / MODEL_WIDTH) + norm_eps)
        gains = gain[...].astype(F32).T
        lane = lax.broadcasted_iota(jnp.int32, gains.shape, 1)
        column = jnp.concatenate(
            [
                jnp.sum(jnp.where(lane == m * (FEATS // 128) + i, gains, 0.0), axis=1, keepdims=True)
                for i in range(FEATS // 128)
            ],
            axis=0,
        )
        normed = (xt[...] * inverse * column).astype(BF)
        for yy in range(NY):
            at[yy, 0] = normed[yy * ROWS : (yy + 1) * ROWS]

    def mask():
        token = lax.broadcasted_iota(jnp.int32, (1, SEQ), 1)
        live = (token < lengths[0]).astype(F32)
        masked = (gin[...].astype(F32).T * live).astype(BF)
        for yy in range(NY):
            at[yy, 1] = masked[yy * ROWS : (yy + 1) * ROWS]

    def tokens_first():
        load(1).wait()
        xt[...] = xin[...].astype(F32).T
        ps[...] = jnp.broadcast_to(jnp.sum(xt[...] * xt[...], axis=0, keepdims=True), ps.shape)
        for k in FAR_FIRST:
            p_copy(k).start()
        load(2).wait()
        load(5).wait()
        assemble(1, adapter_rows(0))
        normalize()
        tokens_start(0)

    def tokens_second():
        load(3).wait()
        mask()
        tokens_start(1)

    def weights_rest():
        load(4).wait()
        load(6).wait()
        assemble(2, adapter_rows(1))
        own_rows()

    def adapters_rest():
        part[...] = jnp.zeros_like(part)
        ad[...] = jnp.zeros_like(ad)
        ad[0, SPOT : SPOT + ADAPTER_RANK, :COLS] = up_b[...]
        ad[1, SPOT : SPOT + ADAPTER_RANK, :COLS] = down_a[...]

    def tile_of(i):
        return pl.ds(pl.multiple_of(i * 128, 128), 128)

    def spots(a):
        return a[SPOT : SPOT + ADAPTER_RANK]

    def forward_side():
        up_latent = c[1, :, LANE0:].astype(BF)
        lat[...] = jnp.zeros_like(lat)

        def chunk(i, carry):
            cols = tile_of(i)
            gate_act = jax.nn.silu(c[0, :, cols])
            c[0, :, cols] = gate_act
            up = c[1, :, cols] + adapter_scale * jnp.dot(up_latent, ad[0, :, cols], preferred_element_type=F32)
            hidden = (gate_act * up).astype(BF)
            hid[:, cols] = hidden
            lat[0] += contract_columns(ad[1, :, cols], hidden)
            return carry

        lax.fori_loop(0, WIDE // 128, chunk, 0)
        v[0] = spots(lat[0]).astype(BF)
        for k in FAR_FIRST:
            v_copy(0, k).start()

    def down_side():
        v_all[0, m] = v[0]
        for k in range(1, NMP):
            v_copy(0, k).wait_recv()
        latent = jnp.sum(v_all[0].astype(F32), axis=0).astype(BF)
        for yy in range(NY):
            put(yy, 4, adapter_scale * contract_columns(latent, at[yy, 1]))

    def backward_side(lo, hi):
        up_latent = c[1, :, LANE0:].astype(BF)
        back_latent = c[2, :, LANE0:].astype(BF)

        def chunk(i, carry):
            cols = tile_of(i)
            back = c[2, :, cols] + adapter_scale * jnp.dot(back_latent, ad[1, :, cols], preferred_element_type=F32)
            up_gradient = (back * c[0, :, cols]).astype(BF)
            lat[1] += contract_columns(ad[0, :, cols], up_gradient)
            full[:ADAPTER_RANK, cols] = adapter_scale * spots(contract_row_dims(back_latent, hid[:, cols]))
            full[ADAPTER_RANK:, cols] = adapter_scale * spots(contract_row_dims(up_latent, up_gradient))
            return carry

        lax.fori_loop(lo, hi, chunk, 0)

    def v_copy(i, k):
        return remote(v.at[i], v_all.at[i, m], vs.at[i, k - 1], vr.at[i, k - 1], d, lax.rem(m + k, NMP))

    def q_copy(k):
        return remote(q, q_all.at[m], qs.at[k - 1], qr.at[k - 1], d, lax.rem(m + k, NMP))

    def put(yy, j0, rows):
        for j in range(4):
            part[(j0 + j) * NY + yy, 8:12] = rows[4 * j : 4 * j + 4, :128]
            part[(j0 + j) * NY + yy, 12:16, : ROWS - 128] = rows[4 * j : 4 * j + 4, 128:]

    plan = {
        1: [tokens_first],
        2: [tokens_second],
        3: [lambda: tokens_x(0)],
        4: [weights_rest],
        5: [adapters_rest],
        6: [lambda: tokens_on(0), lambda: tokens_x(1)],
        9: [lambda: tokens_last(0)],
        10: [lambda: ring_finish(0), lambda: tokens_done(0), lambda: unit_far(0)],
        11: [lambda: unit_near(0, 0)],
        12: [lambda: unit_near(0, 1)],
        13: [lambda: tokens_on(1), lambda: unit_pass(0)],
        14: [lambda: unit_own(0)],
        15: [lambda: tokens_last(1)],
        18: [lambda: ring_finish(1), lambda: unit_far(1)],
        19: [lambda: unit_near(1, 0)],
        20: [lambda: unit_near(1, 1)],
        21: [lambda: unit_sum(0)],
        22: [lambda: unit_pass(1)],
        23: [lambda: unit_own(1), lambda: tokens_done(1)],
        25: [lambda: ring_finish(2), lambda: unit_far(2)],
        26: [lambda: unit_near(2, 0)],
        27: [lambda: unit_near(2, 1)],
    }
    for at_position, (p, i) in enumerate(ORDER):
        ring_issue(p, i)
        for u in plan.get(at_position, ()):
            u()
    ring_finish(3)
    unit_far(3)
    unit_pass(2)
    unit_near(3, 0)
    unit_near(3, 1)
    unit_own(2)
    unit_own(3)
    unit_pass(3)
    unit_sum(1)
    forward_side()
    unit_sum(2)
    backward_side(3, WIDE // 128)
    unit_sum(3)
    backward_side(0, 3)
    v[1] = spots(lat[1]).astype(BF)
    for k in FAR_FIRST:
        v_copy(1, k).start()
    v_all[1, m] = v[1]
    down_side()

    for i in range(NDP):
        for r in range(4):
            part[i, :8, r * 32 : r * 32 + 32] = full[r * 8 : r * 8 + 8, i * SHARE : i * SHARE + 32]
    squares = jnp.sum(full[...] * full[...], keepdims=True)
    for k in range(1, NMP):
        v_copy(1, k).wait_recv()
    latent = jnp.sum(v_all[1].astype(F32), axis=0).astype(BF)
    for yy in range(NY):
        put(yy, 0, adapter_scale * contract_columns(latent, at[yy, 0]))
    features = part[:, 8:, :]
    squares = squares + jnp.sum(jnp.sum(features * features, axis=0), keepdims=True)
    q[...] = jnp.broadcast_to(squares, q.shape)
    for k in FAR_FIRST:
        q_copy(k).start()
    q_all[m] = q[...]
    msg[...] = part[...].astype(BF)

    def m_copy(k):
        dd = lax.rem(d + k, NDP)
        return remote(msg.at[dd], msg_all.at[d], ms.at[k], mr.at[d], dd, m)

    def m_arrive(k, carry):
        dd = lax.rem(d + k, NDP)
        remote(msg.at[0], msg_all.at[dd], ms.at[k], mr.at[dd], dd, m).wait_recv()
        remote(factor, factor_all.at[dd], fs.at[k], fr.at[dd], dd, m).wait_recv()
        return carry

    for i in range(NDP - 1):
        m_copy((i + 12) % (NDP - 1) + 1).start()
    msg_all[d] = msg[d]
    for k in range(1, NMP):
        q_copy(k).wait_recv()
    clip_limit = clip_coefficient * math.sqrt(2.0 * ADAPTER_RANK * (MODEL_WIDTH + HIDDEN_SHARD))
    norm = jnp.sqrt(jnp.sum(q_all[...], axis=0))
    factor[...] = jnp.minimum(1.0, clip_limit / (norm + 1e-06))[:1]

    def f_copy(k):
        dd = lax.rem(d + k, NDP)
        return remote(factor, factor_all.at[d], fs.at[k], fr.at[d], dd, m)

    for i in range(NDP - 1):
        f_copy((i + 12) % (NDP - 1) + 1).start()
    factor_all[d] = factor[...]
    lax.fori_loop(1, NDP, m_arrive, 0)
    summed = jnp.sum(msg_all[...].astype(F32) * factor_all[...], axis=0)
    us[...] = summed[8:]

    goal = m * NY + y
    here = z == m

    def u_copy(k):
        return remote(us, u_row.at[z], us4.at[k], ur4.at[z], goal, lax.rem(m + k, NMP))

    for k in range(1, NMP):
        u_copy(k).start()

    @pl.when(jnp.logical_not(here))
    def _():
        u_copy(0).start()

    @pl.when(here)
    def _():
        u_row[z] = us[...]

    for r in range(4):
        s_out[r * 8 : r * 8 + 8] = summed[:8, r * 32 : r * 32 + SHARE]

    for j in range(NZ):
        @pl.when(jnp.logical_not(jnp.logical_and(here, z == j)))
        def _():
            remote(us, u_row.at[j], us4.at[0], ur4.at[j], goal, lax.rem(m + 1, NMP)).wait_recv()

        u_out[4 * j : 4 * j + 4, :128] = u_row[j, :4]
        u_out[4 * j : 4 * j + 4, 128:] = u_row[j, 4:, : ROWS - 128]

    def m_sent(k, carry):
        m_copy(k).wait_send()
        f_copy(k).wait_send()
        return carry

    lax.fori_loop(1, NDP, m_sent, 0)
    for k in range(1, NMP):
        v_copy(0, k).wait_send()
        v_copy(1, k).wait_send()
        q_copy(k).wait_send()
        u_copy(k).wait_send()

    @pl.when(jnp.logical_not(here))
    def _():
        u_copy(0).wait_send()

    for p in range(4):
        for way in range(2):
            for i in range(7):
                ring_copy(p, way, i).wait_send()
            half_copy(p, way).wait_send()
            for h in range(2):
                full_copy(p, way, h).wait_send()
    for a in range(2):
        for k in (1, 2, 3):
            y_copy(a, k).wait_send()
        for i in range(4):
            x_copy(a, i).wait_send()
        for i in range(5):
            core_copy(a, i).wait_send()
    for k in range(1, NMP):
        p_copy(k).wait_send()


def gradients(lengths, x, g, wg, wu, wd, up_a, down_b, gain, up_b, down_a):
    vmem = pl.BlockSpec(memory_space=pltpu.VMEM)
    dma = pltpu.SemaphoreType.DMA
    return pl.pallas_call(
        gradients_kernel,
        out_shape=(
            jax.ShapeDtypeStruct((2 * ADAPTER_RANK, ROWS), F32),
            jax.ShapeDtypeStruct((2 * ADAPTER_RANK, SHARE), F32),
        ),
        in_specs=[pl.BlockSpec(memory_space=pltpu.SMEM), *[pl.BlockSpec(memory_space=pl.ANY)] * 7, *[vmem] * 3],
        out_specs=(vmem, vmem),
        scratch_shapes=[
            pltpu.VMEM((SEQ, FEATS), BF),
            pltpu.VMEM((SEQ, FEATS), BF),
            pltpu.VMEM((3, ROWS, COLS), BF),
            pltpu.VMEM((2, ADAPTER_RANK, SEQ), BF),
            pltpu.VMEM((128, SEQ), F32),
            pltpu.VMEM((2, 128, WIDE), BF),
            dma((7,)),
            pltpu.VMEM((3, SEQ, WIDE), F32),
            pltpu.VMEM((NY, 2, ROWS, SEQ), BF),
            pltpu.VMEM((3, ROWS, WIDE), BF),
            pltpu.VMEM((FEATS, SEQ), F32),
            pltpu.VMEM((NY, 2, KLEN, SEQ), BF),
            pltpu.VMEM((3, KLEN, WIDE), BF),
            pltpu.VMEM((3, 2, 128, WIDE), BF),
            pltpu.VMEM((3, 2, SEQ, WIDE), BF),
            pltpu.VMEM((3, 2, 128, WIDE), F32),
            pltpu.VMEM((3, 2, 128, WIDE), BF),
            pltpu.VMEM((3, 2, SEQ, WIDE), BF),
            pltpu.VMEM((8, SEQ), F32),
            pltpu.VMEM((NMP, 8, SEQ), F32),
            pltpu.VMEM((2, 128, SEQ), F32),
            pltpu.VMEM((SEQ, WIDE), BF),
            pltpu.VMEM((2 * ADAPTER_RANK, WIDE), F32),
            pltpu.VMEM((2, ADAPTER_RANK, SEQ), BF),
            pltpu.VMEM((2, NMP, ADAPTER_RANK, SEQ), BF),
            pltpu.VMEM((8, 128), F32),
            pltpu.VMEM((NMP, 8, 128), F32),
            pltpu.VMEM((NDP, 16, 128), F32),
            pltpu.VMEM((NDP, 16, 128), BF),
            pltpu.VMEM((NDP, 16, 128), BF),
            pltpu.VMEM((1, 128), F32),
            pltpu.VMEM((NDP, 1, 128), F32),
            pltpu.VMEM((8, 128), F32),
            pltpu.VMEM((NZ, 8, 128), F32),
            dma((4, 2, 7)),
            dma((4, 2, 7)),
            dma((2, 3)),
            dma((2, 3)),
            dma((2,)),
            dma((2, 4)),
            dma((2, 4)),
            dma((2, 5)),
            dma((2, 5)),
            dma((4, 2)),
            dma((4, 2)),
            dma((4, 2, 2)),
            dma((4, 2, 2)),
            dma((NMP - 1,)),
            dma((NMP - 1,)),
            dma((2, NMP - 1)),
            dma((2, NMP - 1)),
            dma((NMP - 1,)),
            dma((NMP - 1,)),
            dma((NDP,)),
            dma((NDP,)),
            dma((NDP,)),
            dma((NDP,)),
            dma((NMP,)),
            dma((NMP,)),
        ],
        compiler_params=pltpu.CompilerParams(collective_id=0, has_side_effects=True),
        name="gradients",
    )(lengths, x, g, wg, wu, wd, up_a, down_b, gain, up_b, down_a)


def hand_over_kernel(u, s, up_a, up_b, down_a, down_b):
    up_a[...] = u[:ADAPTER_RANK]
    down_b[...] = u[ADAPTER_RANK:]
    down_a[...] = s[:ADAPTER_RANK]
    up_b[...] = s[ADAPTER_RANK:]


def hand_over(u, s):
    vmem = pl.BlockSpec(memory_space=pltpu.VMEM)
    of_u = jax.ShapeDtypeStruct((ADAPTER_RANK, ROWS), F32)
    of_s = jax.ShapeDtypeStruct((ADAPTER_RANK, SHARE), F32)
    return pl.pallas_call(
        hand_over_kernel, out_shape=(of_u, of_s, of_s, of_u), in_specs=[vmem] * 2, out_specs=(vmem,) * 4, name="hand_over"
    )(u, s)


def per_device(
    residual_input,
    cotangent,
    lengths,
    norm_gain_vector,
    gate_projection_weight,
    up_projection_weight,
    down_projection_weight,
    up_adapter_first,
    up_adapter_second,
    down_adapter_first,
    down_adapter_second,
):
    u, s = gradients(
        lengths,
        residual_input,
        cotangent,
        gate_projection_weight,
        up_projection_weight,
        down_projection_weight,
        up_adapter_first.T,
        down_adapter_second,
        norm_gain_vector.reshape(MODEL_WIDTH // 128, 128),
        up_adapter_second,
        down_adapter_first.T,
    )
    up_a, up_b, down_a, down_b = hand_over(u, s)
    return (up_a.T, up_b, down_a.T, down_b)


def solution(mesh):
    return jax.shard_map(
        per_device,
        mesh=mesh,
        in_specs=(
            P("dp", "mp"),
            P("dp", "mp"),
            P("dp"),
            P(),
            P("dp", "mp"),
            P("dp", "mp"),
            P("dp", "mp"),
            P(),
            P(None, "mp"),
            P("mp", None),
            P(),
        ),
        out_specs=(P("dp", None), P(None, ("mp", "dp")), P(("mp", "dp"), None), P(None, "dp")),
        check_vma=False,
    )
```
